256 devices in a mesh: band: 64 (over x, y, z_hi, core), chan: 4 (over z_lo).
Axes of the slice: x: 4, y: 4, z: 8 (z_hi: 2, z_lo: 4; z = z_hi * 4 + z_lo), core: 2. Of those that a mesh axis runs over, the one named last changes fastest.
Arguments:
- cells_next: bfloat16 [131072, 1024], P('band', 'chan'), may hold values from -6 to 6
- node_embed: bfloat16 [16384, 1024], P('band', 'chan'), may hold values from -6 to 6
- enc_mix: bfloat16 [1024, 1024], P(None, 'chan'), may hold values from -0.1875 to 0.1875
- out_cotangent: bfloat16 [131072, 1024], P('band', 'chan'), may hold values from -16 to 16
- decoded_saved: bfloat16 [131072, 1024], P('band', 'chan'), may hold values from -6 to 6
- dec_proj: bfloat16 [1024, 1024], P(None, 'chan'), may hold values from -0.1875 to 0.1875
- tile_source: int32 [128, 16], replicated, may hold values from 0 to 1023, as said below
- tile_codes: int32 [128, 16, 128, 128], P('band'), may hold values from 0 to 65535
Outputs:
- hidden_nodes: bfloat16 [16384, 1024], P('band', 'chan')
- node_grad: bfloat16 [16384, 1024], P('band', 'chan')
- w_dec_grad: float32 [1024, 1024], P('band', 'chan')
The draws below stay inside these ranges and needn't reach their ends.
Inputs may be any that keep to these rules, and one draw needn't show every extreme that they name: `tile_source`: each entry is a cell block; cell block c lies in band c // 16 and node block n in band n // 2. The cell blocks of a node block's tiles lie within 3 bands of its own. Of the 32 tiles of one band's node blocks, exactly 8 read that band itself and at most 8 read any other one band.
All inputs are finite; a program needn't handle non-finite values.
Results may differ from the reference program's by a relative error of at most 0.0049.
Values may be sent and summed in bfloat16 or wider, within the bound.
A program may use at most 64 MiB of HBM per device.

```python
import jax
import jax.numpy as jnp
from jax import lax

D = 1024
BLK = 128
K = 16
R = 3
CB_DEV = 16
NB_DEV = 2
CAP = 8
NODE_BLOCKS = 128
CELLS = 131072
NODES = 16384


def draw_tile_source(key, part):
    band_total = NODE_BLOCKS // NB_DEV
    tile_total = NB_DEV * K
    pool_size = 2 * R * CAP

    def one_band(band_key, owner):
        score_key, shuffle_key, local_key = jax.random.split(band_key, 3)
        tokens = jnp.arange(pool_size, dtype=jnp.int32)
        neighbour = tokens // CAP
        offset = jnp.where(neighbour < R, neighbour - R, neighbour - R + 1)
        source = owner + offset
        usable = (source >= 0) & (source < band_total)
        scores = jax.random.randint(score_key, (pool_size,), 0, 1 << 20, dtype=jnp.int32) * pool_size + tokens
        scores = jnp.where(usable, scores, (1 << 30) + tokens)
        ranking = jnp.argsort(scores)
        picked = source[ranking[:tile_total - CAP]]
        bands_drawn = jnp.concatenate([jnp.full((CAP,), owner, jnp.int32), picked.astype(jnp.int32)])
        shuffle = jax.random.permutation(shuffle_key, tile_total)
        local_block = jax.random.randint(local_key, (tile_total,), 0, CB_DEV, dtype=jnp.int32)
        return (bands_drawn[shuffle] * CB_DEV + local_block).reshape(NB_DEV, K)
    band_keys = jax.random.split(key, band_total)
    drawn = jax.vmap(one_band)(band_keys, jnp.arange(band_total, dtype=jnp.int32))
    return drawn.reshape(band_total * NB_DEV, K).astype(jnp.int32)


def plant(array, rng, smallest, high):
    extent = array.shape
    place = [jax.random.randint(jax.random.fold_in(rng, axis), (), 0, extent[axis]) for axis in range(len(extent))]
    array = array.at[tuple(place)].set(smallest)
    longest = extent.index(max(extent))
    place[longest] = (place[longest] + 1) % extent[longest]
    return array.at[tuple(place)].set(high)


def spiked(result, own_key, source, target, shards_of, factor):
    owner, partner = [(jnp.arange(result.shape[position]) // (result.shape[position] // shards_of)).reshape([-1 if axis == position else 1 for axis in range(result.ndim)]) for position in (source, target)]
    chosen = jax.random.permutation(own_key, shards_of)[partner]
    strong = (owner == chosen) | (owner == (partner + shards_of // 2) % shards_of)
    return jnp.where(strong, factor * result, result)


def shard_levels(own_key, shape, shards, smallest, top_value):
    level = 1.0
    for axis_at, parts in shards:
        steps = jax.random.uniform(jax.random.fold_in(jax.random.fold_in(own_key, 6), axis_at), (parts,), jnp.float32, smallest / len(shards), top_value / len(shards))
        level = level * jnp.repeat(jnp.exp(steps), shape[axis_at] // parts).reshape((-1,) + (1,) * (len(shape) - 1 - axis_at))
    return level


def noise(rng, shape, scale, reach, shards=(), kind=jnp.bfloat16):
    values = scale * jax.random.normal(rng, shape, jnp.float32)
    if shards:
        values = values * shard_levels(rng, shape, shards, -0.22, 0.18)
    return jnp.clip(values, -reach, reach).astype(kind)


def heavy_noise(stream_key, extent, spread, limit, cuts, heavy, held_as=jnp.bfloat16):
    entries = spread * jax.random.normal(stream_key, extent, jnp.float32)
    if cuts:
        entries = entries * shard_levels(stream_key, extent, cuts, -0.22, 0.18)
    return jnp.clip(spiked(entries, jax.random.fold_in(stream_key, 3), *heavy), -limit, limit).astype(held_as)


def setup_inputs(seed: int = 0) -> dict:
    arg_keys = jax.random.split(jax.random.key(seed), 9)
    cells_next = noise(arg_keys[0], (CELLS, D), 1.0, 6.0, ((0, 64), (1, 4)))
    node_embed = noise(arg_keys[1], (NODES, D), 1.0, 6.0, ((0, 64), (1, 4)))
    enc_mix = noise(arg_keys[2], (D, D), D ** -0.5, 0.1875, ((1, 4),))
    out_cotangent = heavy_noise(arg_keys[3], (CELLS, D), 1.0, 16.0, ((0, 64), (1, 4)), (0, 1, 64, 4.0))
    decoded_saved = noise(arg_keys[4], (CELLS, D), 1.0, 6.0, ((0, 64), (1, 4)))
    dec_proj = noise(arg_keys[5], (D, D), D ** -0.5, 0.1875, ((1, 4),))
    tile_source = draw_tile_source(jax.random.fold_in(arg_keys[8], 71), 0)
    tile_codes = plant(jax.random.randint(arg_keys[7], (NODE_BLOCKS, K, BLK, BLK), 0, 65536), jax.random.fold_in(arg_keys[7], 1), 0, 65535).astype(jnp.int32)
    return {"cells_next": cells_next, "node_embed": node_embed, "enc_mix": enc_mix, "out_cotangent": out_cotangent, "decoded_saved": decoded_saved, "dec_proj": dec_proj, "tile_source": tile_source, "tile_codes": tile_codes}


def split_codes(code_words):
    low_codes = (code_words % 256 - 128).astype(jnp.bfloat16)
    high_codes = (code_words // 256 - 128).astype(jnp.bfloat16)
    return low_codes, high_codes


def reference(cells_next, node_embed, enc_mix, out_cotangent, decoded_saved, dec_proj, tile_source, tile_codes):
    tile_scale = (3.0 / (K * BLK)) ** 0.5 / 128.0
    channels = cells_next.shape[1]
    cotangent_wide = out_cotangent.astype(jnp.float32)
    cell_grad = jnp.dot(cotangent_wide, dec_proj.astype(jnp.float32), preferred_element_type=jnp.float32).astype(jnp.bfloat16)
    cell_blocks = cells_next.reshape(-1, BLK, channels)
    grad_blocks = cell_grad.reshape(-1, BLK, channels)

    def per_block(inputs):
        sources, code_words = inputs
        enc_tile, dec_tile = split_codes(code_words)
        gathered = cell_blocks[sources].astype(jnp.float32)
        aggregate = jnp.einsum("kab,kbd->ad", enc_tile.astype(jnp.float32), gathered) * tile_scale
        grad_rows = grad_blocks[sources].astype(jnp.float32)
        node_part = jnp.einsum("kab,kbd->ad", dec_tile.astype(jnp.float32), grad_rows) * tile_scale
        return aggregate.astype(jnp.bfloat16), node_part.astype(jnp.bfloat16)

    agg_blocks, node_blocks = lax.map(per_block, (tile_source, tile_codes))
    aggregate = agg_blocks.reshape(-1, channels)
    mixed_rows = jnp.dot(aggregate, enc_mix, preferred_element_type=jnp.float32)
    hidden_nodes = (node_embed.astype(jnp.float32) + jax.nn.silu(mixed_rows)).astype(jnp.bfloat16)
    node_grad = node_blocks.reshape(-1, channels)
    w_dec_grad = jnp.dot(cotangent_wide.T, decoded_saved.astype(jnp.float32), preferred_element_type=jnp.float32) * (CELLS ** -0.5)
    return hidden_nodes, node_grad, w_dec_grad
```

```python
import jax
import jax.numpy as jnp
from jax import lax
from jax.experimental import pallas as pl
from jax.experimental.pallas import tpu as pltpu
from jax.sharding import PartitionSpec as P

BLK = 128
K = 16
NB_DEV = 2
CHIPS = 32
TILES = NB_DEV * K
SLOTS = 16
T2 = 8
CH = 256
ROWS = 2048
QROWS = 512
NODES = 256
SCALE = (3.0 / (K * BLK)) ** 0.5 / 128.0
MESH = pl.DeviceIdType.MESH
BF = jnp.bfloat16
F32 = jnp.float32

UP = (0, 4, 16, 20)
DOWN = (8, 12, 24, 28)
CHUNK = 4


def chip_links(chip, z_hi, core):
    side = 1 - 2 * z_hi
    across = chip + side
    beyond = (chip - side + CHIPS) % CHIPS
    relay_to = (chip + 2 * side + CHIPS) % CHIPS
    two_to = (chip + 4 * core - 2 + CHIPS) % CHIPS
    two_from = (chip - 4 * core + 2 + CHIPS) % CHIPS
    return across, beyond, relay_to, two_to, two_from


def slot_tables(tile_source, my_band):
    chip, core = my_band // 2, my_band % 2
    across, beyond, _, two_to, two_from = chip_links(chip, chip % 2, core)
    targets = jnp.stack(
        [my_band] * 4 + [2 * beyond + core, 2 * across + core, 2 * two_from + core, my_band]
    )
    sources = jnp.stack([beyond, across, two_to, chip, chip, chip, chip, chip])
    blocks = tile_source.reshape(-1, TILES)[targets]
    tile = jnp.arange(TILES, dtype=jnp.int32)
    match = (blocks // 32) == sources[:, None]
    before = tile[None, :, None] > tile[None, None, :]
    rank = jnp.sum((match[:, None, :] & before).astype(jnp.int32), axis=2)
    sending = (jnp.arange(8) < 4)[:, None]
    entry = jnp.where(sending, tile[None, :] + 256, blocks % 32 + 256 * (tile[None, :] // K))
    slot = jnp.arange(SLOTS, dtype=jnp.int32)
    chosen = match[:, :, None] & (rank[:, :, None] == slot[None, None, :])
    return jnp.sum(jnp.where(chosen, entry[:, :, None], 0), axis=1)


def kernel(
    table,
    cells_hbm,
    embed_hbm,
    mix_hbm,
    cot_hbm,
    saved_hbm,
    proj_hbm,
    codes_hbm,
    hidden_out,
    grad_out,
    w_out,
    codes,
    cells,
    cot,
    cot_all,
    saved_all,
    mix,
    proj,
    embed,
    packed,
    own_packed,
    got_z,
    got_y,
    got_two,
    lhs,
    rhs,
    own_sum,
    part_send,
    part_recv,
    agg_all,
    w_part,
    core_recv,
    y_own,
    y_send,
    y_recv,
    x_send,
    x_recv,
    z_send,
    z_recv,
    load_sem,
    share_send,
    share_recv,
    up_send,
    up_recv,
    down_send,
    down_recv,
    relay_send,
    relay_recv,
    two_send,
    two_recv,
    a_send,
    a_recv,
    core_send_sem,
    core_recv_sem,
    y_send_sem,
    y_recv_sem,
    x_send_sem,
    x_recv_sem,
    z_send_sem,
    z_recv_sem,
    part_send_sem,
    part_recv_sem,
    agg_send_sem,
    agg_recv_sem,
):
    band = lax.axis_index("band")
    q = lax.axis_index("chan")
    core = band % 2
    chip = band // 2
    h = chip % 2
    y = (band // 4) % 4
    x = band // 16
    across, beyond, relay_to, two_to, two_from = chip_links(chip, h, core)

    def at_chip(other_chip, chan):
        return (2 * other_chip + core, chan)

    def remote(src, dst, send, recv, device):
        return pltpu.make_async_remote_copy(
            src_ref=src,
            dst_ref=dst,
            send_sem=send,
            recv_sem=recv,
            device_id=device,
            device_id_type=MESH,
        )

    sibling = (band + 1 - 2 * core, q)
    across_q = [at_chip(across, (q + d) % 4) for d in range(4)]
    along_q = [(band, (q + d) % 4) for d in range(1, 4)]
    along_y = [(x * 16 + ((y + d) % 4) * 4 + h * 2 + core, q) for d in range(1, 4)]
    along_x = [(((x + d) % 4) * 16 + y * 4 + h * 2 + core, q) for d in range(1, 4)]

    barrier = pltpu.get_barrier_semaphore()
    partners = (
        [sibling]
        + across_q
        + along_q
        + along_y
        + along_x
        + [at_chip(two_to, q), at_chip(two_from, q), at_chip(beyond, q)]
    )
    for partner in partners:
        pl.semaphore_signal(barrier, inc=1, device_id=partner, device_id_type=MESH)

    loads = [
        pltpu.make_async_copy(codes_hbm, codes, load_sem.at[0]),
        pltpu.make_async_copy(cells_hbm, cells.at[core], load_sem.at[1]),
        pltpu.make_async_copy(cot_hbm, cot.at[core], load_sem.at[2]),
        pltpu.make_async_copy(cot_hbm.at[q], cot_all.at[q], load_sem.at[3]),
        pltpu.make_async_copy(saved_hbm.at[q], saved_all.at[q], load_sem.at[4]),
        pltpu.make_async_copy(mix_hbm, mix, load_sem.at[5]),
        pltpu.make_async_copy(proj_hbm, proj, load_sem.at[6]),
        pltpu.make_async_copy(embed_hbm, embed, load_sem.at[7]),
    ]
    for load in loads:
        load.start()

    def pack(row, count, dest, base):
        def one(s, carry):
            item = table[row, s]
            words = codes[item & 31]
            low = ((words & 255) - 128).astype(F32)
            high = ((words >> 8) - 128).astype(F32)
            keep = jnp.where(item >= 256, 1.0, 0.0).astype(F32)
            dest[base + s, 0] = (low * keep).astype(BF)
            dest[base + s, 1] = (high * keep).astype(BF)
            return carry

        lax.fori_loop(0, count, one, 0)

    loads[0].wait()
    pack(0, SLOTS, packed, 0)
    pack(1, SLOTS, packed, 16)
    pack(2, T2, packed, 32)
    pl.semaphore_wait(barrier, len(partners))

    z_up = at_chip(jnp.where(q == 3, across, chip), (q + 1) % 4)
    z_down = at_chip(jnp.where(q == 0, across, chip), (q + 3) % 4)

    def up_copy(step, src):
        part = pl.ds(UP[step], CHUNK)
        return remote(src.at[part], got_z.at[part], up_send.at[step], up_recv.at[step], z_up)

    def down_copy(step, src):
        part = pl.ds(DOWN[step], CHUNK)
        return remote(src.at[part], got_z.at[part], down_send.at[step], down_recv.at[step], z_down)

    def relay_copy(index, start):
        part = pl.ds(start, CHUNK)
        return remote(
            got_z.at[part],
            got_y.at[part],
            relay_send.at[index],
            relay_recv.at[index],
            at_chip(relay_to, q),
        )

    relays = [
        relay_copy(index, start)
        for index, start in enumerate((UP[0], DOWN[0], UP[1], DOWN[1]))
    ]
    for step in range(4):

        @pl.when(q == 3)
        def _(step=step):
            up_copy(step, packed).start()

        @pl.when(q == 0)
        def _(step=step):
            down_copy(step, packed).start()

    two = remote(packed.at[pl.ds(32, T2)], got_two, two_send, two_recv, at_chip(two_to, q))
    two.start()
    shares = [
        remote(cells_hbm, cells.at[core], share_send.at[0], share_recv.at[0], sibling),
        remote(cot_hbm, cot.at[core], share_send.at[1], share_recv.at[1], sibling),
    ]
    for share in shares:
        share.start()

    a_copies = []
    for d in range(1, 4):
        other = (q + d) % 4
        for array, (src, dst) in enumerate(((cot_hbm, cot_all), (saved_hbm, saved_all))):
            index = 2 * (d - 1) + array
            a_copies.append(
                remote(src.at[other], dst.at[q], a_send.at[index], a_recv.at[index], (band, other))
            )
    waiting = list(a_copies)

    for step in range(4):
        up_copy(step, got_z).wait_recv()

        @pl.when(q < 3)
        def _(step=step):
            up_copy(step, got_z).start()

        down_copy(step, got_z).wait_recv()

        @pl.when(q > 0)
        def _(step=step):
            down_copy(step, got_z).start()

        if step < 2:
            relays[2 * step].start()
            relays[2 * step + 1].start()
        for _ in range(1 if step < 2 else 2):
            waiting.pop(0).start()

    def sums(row, count, tiles, base):
        def one(s, carry):
            item = table[row, s]
            column = pl.ds(pl.multiple_of(s * BLK, BLK), BLK)
            first = jnp.where(item < 256, 1.0, 0.0).astype(BF)
            second = jnp.where(item < 256, 0.0, 1.0).astype(BF)
            for which in range(2):
                tile = tiles[base + s, which]
                lhs[which, pl.ds(0, BLK), column] = tile * first
                lhs[which, pl.ds(BLK, BLK), column] = tile * second
            block = item & 31
            rhs[0, column, :] = cells[block // 16, (block // 4) % 4, block % 4]
            rhs[1, column, :] = cot[block // 16, (block // 4) % 4, block % 4]
            return carry

        lax.fori_loop(0, count, one, 0)
        depth = count * BLK
        return [
            jnp.dot(
                lhs[which, :, pl.ds(0, depth)],
                rhs[which, pl.ds(0, depth), :],
                preferred_element_type=F32,
            )
            for which in range(2)
        ]

    for load in loads[1:3]:
        load.wait()
    for share in shares:
        share.wait_recv()

    part_to = [at_chip(across, q), at_chip(two_from, q), at_chip(beyond, q)]
    part_copies = [
        remote(
            part_send.at[g], part_recv.at[g], part_send_sem.at[g], part_recv_sem.at[g], part_to[g]
        )
        for g in range(3)
    ]

    def send_part(g, row, count, tiles, base):
        result = sums(row, count, tiles, base)
        for which in range(2):
            part_send[g, which] = result[which].astype(BF)
        part_copies[g].start()

    send_part(0, 5, SLOTS, got_z, 16)
    two.wait_recv()
    send_part(1, 6, T2, got_two, 0)
    for copy in relays:
        copy.wait_recv()
    send_part(2, 4, SLOTS, got_y, 0)
    pack(3, SLOTS, own_packed, 0)
    result = sums(7, SLOTS, own_packed, 0)
    for which in range(2):
        own_sum[which] = result[which]

    for load in loads[3:5]:
        load.wait()
    for copy in a_copies:
        copy.wait_recv()

    core_copies = [
        remote(
            w_part.at[d, 1 - core],
            core_recv.at[d],
            core_send_sem.at[d],
            core_recv_sem.at[d],
            sibling,
        )
        for d in range(4)
    ]
    order = (1, 2, 3, 0)
    for d in order:
        left = cot_all.at[(x + d) % 4]

        def columns(j, carry, d=d, left=left):
            product = lax.dot_general(
                left[...].reshape(QROWS, CH),
                saved_all[j].reshape(QROWS, CH),
                (((0,), (0,)), ((), ())),
                preferred_element_type=F32,
            )
            span = pl.ds(pl.multiple_of(j * CH, CH), CH)
            for group in range(8):
                for half in range(2):
                    start = (2 * group + half) * 16
                    w_part[d, half, group // 2, pl.ds((group % 2) * 16, 16), span] = product[
                        start : start + 16
                    ]
            return carry

        lax.fori_loop(0, 4, columns, 0)
        core_copies[d].start()

    y_copies = {}
    for d in order:
        core_copies[d].wait_recv()
        for yy in range(4):
            total = w_part[d, core, yy] + core_recv[d, yy]
            y_own[d, yy] = total
            y_send[d, yy] = total.astype(BF)
        for e in range(1, 4):
            y_copies[d, e] = remote(
                y_send.at[d, (y + e) % 4],
                y_recv.at[d, e - 1],
                y_send_sem.at[d, e - 1],
                y_recv_sem.at[d, e - 1],
                along_y[e - 1],
            )
            y_copies[d, e].start()

    for copy in part_copies:
        copy.wait_recv()
    for which in range(2):
        total = own_sum[which]
        for g in range(3):
            total = total + part_recv[g, which].astype(F32)
        agg_all[q, which] = (total * SCALE).astype(BF)
    agg_copies = [
        remote(
            agg_all.at[q], agg_all.at[q], agg_send_sem.at[d], agg_recv_sem.at[d], along_q[d]
        )
        for d in range(3)
    ]
    for copy in agg_copies:
        copy.start()

    x_copies = {}
    for d in order:
        total = y_own[d, y]
        for e in range(1, 4):
            y_copies[d, e].wait_recv()
            total = total + y_recv[d, e - 1].astype(F32)
        if d > 0:
            x_send[d - 1] = total.astype(BF)
            x_copies[d] = remote(
                x_send.at[d - 1],
                x_recv.at[d - 1],
                x_send_sem.at[d - 1],
                x_recv_sem.at[d - 1],
                along_x[d - 1],
            )
            x_copies[d].start()
    for d in range(1, 4):
        x_copies[d].wait_recv()
        total = total + x_recv[d - 1].astype(F32)
    for hh in range(2):
        for qq in range(4):
            z_send[hh, qq] = total[hh * 16 : hh * 16 + 16, qq * CH : qq * CH + CH]
    z_copies = []
    for hd in range(2):
        for qd in range(4):
            if hd + qd > 0:
                index = hd * 4 + qd - 1
                chan = (q + qd) % 4
                device = at_chip(across, chan) if hd else (band, chan)
                to_h = 1 - h if hd else h
                z_copies.append(
                    remote(
                        z_send.at[to_h, chan],
                        z_recv.at[index],
                        z_send_sem.at[index],
                        z_recv_sem.at[index],
                        device,
                    )
                )
    for copy in z_copies:
        copy.start()

    for load in loads[5:8]:
        load.wait()
    for copy in agg_copies:
        copy.wait_recv()
    mixed = jnp.zeros((NODES, CH), F32)
    grad = jnp.zeros((NODES, CH), F32)
    for j in range(4):
        mixed = mixed + jnp.dot(
            agg_all[j, 0], mix[pl.ds(j * CH, CH), :], preferred_element_type=F32
        )
    hidden_out[...] = (embed[...].astype(F32) + mixed / (1.0 + jnp.exp(-mixed))).astype(BF)
    for j in range(4):
        grad = grad + jnp.dot(
            agg_all[j, 1], proj[pl.ds(j * CH, CH), :], preferred_element_type=F32
        )
    grad_out[...] = grad.astype(BF)

    total = z_send[h, q]
    for index, copy in enumerate(z_copies):
        copy.wait_recv()
        total = total + z_recv[index]
    w_out[...] = total * (ROWS * 64) ** (-0.5)

    for step in range(4):
        up_copy(step, got_z).wait_send()
        down_copy(step, got_z).wait_send()
    two.wait_send()
    ends = relays + shares + a_copies + part_copies + core_copies + agg_copies + z_copies
    for copy in ends + list(y_copies.values()) + list(x_copies.values()):
        copy.wait_send()


def shards(
    cells_next, node_embed, enc_mix, out_cotangent, decoded_saved, dec_proj, tile_source, tile_codes
):
    my_band = lax.axis_index("band")
    table = slot_tables(tile_source, my_band)
    hbm = pl.BlockSpec(memory_space=pl.ANY)
    vmem = pl.BlockSpec(memory_space=pltpu.VMEM)
    dma = pltpu.SemaphoreType.DMA
    scratch = [
        pltpu.VMEM((TILES, BLK, BLK), jnp.int32),
        pltpu.VMEM((2, 4, 4, BLK, CH), BF),
        pltpu.VMEM((2, 4, 4, BLK, CH), BF),
        pltpu.VMEM((4, 4, BLK, CH), BF),
        pltpu.VMEM((4, 4, BLK, CH), BF),
        pltpu.VMEM((4 * CH, CH), BF),
        pltpu.VMEM((4 * CH, CH), BF),
        pltpu.VMEM((NODES, CH), BF),
        pltpu.VMEM((2 * SLOTS + T2, 2, BLK, BLK), BF),
        pltpu.VMEM((SLOTS, 2, BLK, BLK), BF),
        pltpu.VMEM((2 * SLOTS, 2, BLK, BLK), BF),
        pltpu.VMEM((SLOTS, 2, BLK, BLK), BF),
        pltpu.VMEM((T2, 2, BLK, BLK), BF),
        pltpu.VMEM((2, NODES, SLOTS * BLK), BF),
        pltpu.VMEM((2, SLOTS * BLK, CH), BF),
        pltpu.VMEM((2, NODES, CH), F32),
        pltpu.VMEM((3, 2, NODES, CH), BF),
        pltpu.VMEM((3, 2, NODES, CH), BF),
        pltpu.VMEM((4, 2, NODES, CH), BF),
        pltpu.VMEM((4, 2, 4, 32, 4 * CH), F32),
        pltpu.VMEM((4, 4, 32, 4 * CH), F32),
        pltpu.VMEM((4, 4, 32, 4 * CH), F32),
        pltpu.VMEM((4, 4, 32, 4 * CH), BF),
        pltpu.VMEM((4, 3, 32, 4 * CH), BF),
        pltpu.VMEM((3, 32, 4 * CH), BF),
        pltpu.VMEM((3, 32, 4 * CH), BF),
        pltpu.VMEM((2, 4, 16, CH), F32),
        pltpu.VMEM((7, 16, CH), F32),
        dma((8,)),
        dma((2,)),
        dma((2,)),
        dma((4,)),
        dma((4,)),
        dma((4,)),
        dma((4,)),
        dma((4,)),
        dma((4,)),
        dma,
        dma,
        dma((6,)),
        dma((6,)),
        dma((4,)),
        dma((4,)),
        dma((4, 3)),
        dma((4, 3)),
        dma((3,)),
        dma((3,)),
        dma((7,)),
        dma((7,)),
        dma((3,)),
        dma((3,)),
        dma((3,)),
        dma((3,)),
    ]
    hidden_nodes, node_grad, w_dec_grad = pl.pallas_call(
        kernel,
        out_shape=(
            jax.ShapeDtypeStruct((NODES, CH), BF),
            jax.ShapeDtypeStruct((NODES, CH), BF),
            jax.ShapeDtypeStruct((16, CH), F32),
        ),
        in_specs=[pl.BlockSpec(memory_space=pltpu.SMEM)] + [hbm] * 7,
        out_specs=(vmem, vmem, vmem),
        scratch_shapes=scratch,
        compiler_params=pltpu.CompilerParams(
            collective_id=0, has_side_effects=True, vmem_limit_bytes=60 * 1024 * 1024
        ),
        name="encode_and_backward",
    )(
        table,
        cells_next.reshape(4, 4, BLK, CH),
        node_embed,
        enc_mix,
        out_cotangent.reshape(4, 4, BLK, CH),
        decoded_saved.reshape(4, 4, BLK, CH),
        dec_proj,
        tile_codes.reshape(TILES, BLK, BLK),
    )
    return hidden_nodes, node_grad, w_dec_grad


def solution(mesh):
    in_specs = (
        P("band", "chan"),
        P("band", "chan"),
        P(None, "chan"),
        P("band", "chan"),
        P("band", "chan"),
        P(None, "chan"),
        P(),
        P("band", None, None, None),
    )
    out_specs = (P("band", "chan"), P("band", "chan"), P("band", "chan"))
    return jax.shard_map(shards, mesh=mesh, in_specs=in_specs, out_specs=out_specs, check_vma=False)
```

```python
import jax
import jax.numpy as jnp
from jax import lax
from jax.experimental import pallas as pl
from jax.experimental.pallas import tpu as pltpu
from jax.sharding import PartitionSpec as P

BLK = 128
K = 16
NB_DEV = 2
CHIPS = 32
TILES = NB_DEV * K
SLOTS = 16
T2 = 8
CH = 256
ROWS = 2048
QROWS = 512
NODES = 256
SCALE = (3.0 / (K * BLK)) ** 0.5 / 128.0
MESH = pl.DeviceIdType.MESH
BF = jnp.bfloat16
F32 = jnp.float32

CHUNK = 2
STEPS = 8
A_TICKS = (1, 3, 5, 7, 8, 9)


def chip_links(chip, z_hi, core):
    side = 1 - 2 * z_hi
    across = chip + side
    beyond = (chip - side + CHIPS) % CHIPS
    relay_to = (chip + 2 * side + CHIPS) % CHIPS
    two_to = (chip + 4 * core - 2 + CHIPS) % CHIPS
    two_from = (chip - 4 * core + 2 + CHIPS) % CHIPS
    return across, beyond, relay_to, two_to, two_from


def slot_tables(tile_source, my_band):
    chip, core = my_band // 2, my_band % 2
    across, beyond, _, two_to, two_from = chip_links(chip, chip % 2, core)
    targets = jnp.stack(
        [my_band] * 4 + [2 * beyond + core, 2 * across + core, 2 * two_from + core, my_band]
    )
    sources = jnp.stack([beyond, across, two_to, chip, chip, chip, chip, chip])
    blocks = tile_source.reshape(-1, TILES)[targets]
    tile = jnp.arange(TILES, dtype=jnp.int32)
    match = (blocks // 32) == sources[:, None]
    before = tile[None, :, None] > tile[None, None, :]
    rank = jnp.sum((match[:, None, :] & before).astype(jnp.int32), axis=2)
    sending = (jnp.arange(8) < 4)[:, None]
    entry = jnp.where(sending, tile[None, :] + 256, blocks % 32 + 256 * (tile[None, :] // K))
    slot = jnp.arange(SLOTS, dtype=jnp.int32)
    chosen = match[:, :, None] & (rank[:, :, None] == slot[None, None, :])
    return jnp.sum(jnp.where(chosen, entry[:, :, None], 0), axis=1)


def kernel(
    table,
    cells_hbm,
    embed_hbm,
    mix_hbm,
    cot_hbm,
    saved_hbm,
    proj_hbm,
    codes_hbm,
    hidden_out,
    grad_out,
    w_out,
    codes,
    cells,
    cot,
    cot_all,
    saved_all,
    mix,
    proj,
    embed,
    packed,
    own_packed,
    got_z,
    got_y,
    got_two,
    lhs,
    rhs,
    own_sum,
    part_send,
    part_recv,
    agg_all,
    w_part,
    core_recv,
    y_own,
    y_send,
    y_recv,
    x_send,
    x_recv,
    z_send,
    z_recv,
    load_sem,
    share_send,
    share_recv,
    up_send,
    up_recv,
    down_send,
    down_recv,
    relay_send,
    relay_recv,
    two_send,
    two_recv,
    a_send,
    a_recv,
    core_send_sem,
    core_recv_sem,
    y_send_sem,
    y_recv_sem,
    x_send_sem,
    x_recv_sem,
    z_send_sem,
    z_recv_sem,
    part_send_sem,
    part_recv_sem,
    agg_send_sem,
    agg_recv_sem,
):
    band = lax.axis_index("band")
    q = lax.axis_index("chan")
    core = band % 2
    chip = band // 2
    h = chip % 2
    y = (band // 4) % 4
    x = band // 16
    across, beyond, relay_to, two_to, two_from = chip_links(chip, h, core)

    def at_chip(other_chip, chan):
        return (2 * other_chip + core, chan)

    def remote(src, dst, send, recv, device):
        return pltpu.make_async_remote_copy(
            src_ref=src,
            dst_ref=dst,
            send_sem=send,
            recv_sem=recv,
            device_id=device,
            device_id_type=MESH,
        )

    sibling = (band + 1 - 2 * core, q)
    across_q = [at_chip(across, (q + d) % 4) for d in range(4)]
    along_q = [(band, (q + d) % 4) for d in range(1, 4)]
    along_y = [(x * 16 + ((y + d) % 4) * 4 + h * 2 + core, q) for d in range(1, 4)]
    along_x = [(((x + d) % 4) * 16 + y * 4 + h * 2 + core, q) for d in range(1, 4)]

    barrier = pltpu.get_barrier_semaphore()
    partners = (
        [sibling]
        + across_q
        + along_q
        + along_y
        + along_x
        + [at_chip(two_to, q), at_chip(two_from, q), at_chip(beyond, q)]
    )
    for partner in partners:
        pl.semaphore_signal(barrier, inc=1, device_id=partner, device_id_type=MESH)

    loads = [
        pltpu.make_async_copy(codes_hbm, codes, load_sem.at[0]),
        pltpu.make_async_copy(cells_hbm, cells.at[core], load_sem.at[1]),
        pltpu.make_async_copy(cot_hbm, cot.at[core], load_sem.at[2]),
        pltpu.make_async_copy(cot_hbm.at[q], cot_all.at[q], load_sem.at[3]),
        pltpu.make_async_copy(saved_hbm.at[q], saved_all.at[q], load_sem.at[4]),
        pltpu.make_async_copy(mix_hbm, mix, load_sem.at[5]),
        pltpu.make_async_copy(proj_hbm, proj, load_sem.at[6]),
        pltpu.make_async_copy(embed_hbm, embed, load_sem.at[7]),
    ]
    for load in loads:
        load.start()

    def pack(row, count, dest, base):
        def one(s, carry):
            item = table[row, s]
            words = codes[item & 31]
            low = ((words & 255) - 128).astype(F32)
            high = ((words >> 8) - 128).astype(F32)
            keep = jnp.where(item >= 256, 1.0, 0.0).astype(F32)
            dest[base + s, 0] = (low * keep).astype(BF)
            dest[base + s, 1] = (high * keep).astype(BF)
            return carry

        lax.fori_loop(0, count, one, 0)

    loads[0].wait()
    pack(0, SLOTS, packed, 0)
    pack(1, SLOTS, packed, 16)
    pack(2, T2, packed, 32)
    pl.semaphore_wait(barrier, len(partners))

    z_up = at_chip(jnp.where(q == 3, across, chip), (q + 1) % 4)
    z_down = at_chip(jnp.where(q == 0, across, chip), (q + 3) % 4)

    def up_part(step):
        return pl.ds(CHUNK * step + 8 * (step // 4), CHUNK)

    def down_part(step):
        return pl.ds(CHUNK * step + 8 * (step // 4) + 8, CHUNK)

    def up_copy(step, src):
        part = up_part(step)
        return remote(src.at[part], got_z.at[part], up_send.at[step], up_recv.at[step], z_up)

    def down_copy(step, src):
        part = down_part(step)
        return remote(src.at[part], got_z.at[part], down_send.at[step], down_recv.at[step], z_down)

    def relay_copy(index, part):
        return remote(
            got_z.at[part],
            got_y.at[part],
            relay_send.at[index],
            relay_recv.at[index],
            at_chip(relay_to, q),
        )

    for step in range(STEPS):

        @pl.when(q == 3)
        def _(step=step):
            up_copy(step, packed).start()

        @pl.when(q == 0)
        def _(step=step):
            down_copy(step, packed).start()

    two = remote(packed.at[pl.ds(32, T2)], got_two, two_send, two_recv, at_chip(two_to, q))
    two.start()
    shares = [
        remote(cells_hbm, cells.at[core], share_send.at[0], share_recv.at[0], sibling),
        remote(cot_hbm, cot.at[core], share_send.at[1], share_recv.at[1], sibling),
    ]
    for share in shares:
        share.start()

    a_copies = []
    for d in range(1, 4):
        other = (q + d) % 4
        for array, (src, dst) in enumerate(((cot_hbm, cot_all), (saved_hbm, saved_all))):
            index = 2 * (d - 1) + array
            a_copies.append(
                remote(src.at[other], dst.at[q], a_send.at[index], a_recv.at[index], (band, other))
            )
    waiting = list(a_copies)

    for tick in range(STEPS + 3):
        up, down = tick - q, tick - 3 + q

        @pl.when((up >= 0) & (up < STEPS))
        def _(step=up):
            up_copy(step, got_z).wait_recv()

            @pl.when(q < 3)
            def _():
                up_copy(step, got_z).start()

            @pl.when(step < 4)
            def _():
                relay_copy(step, up_part(step)).start()

        @pl.when((down >= 0) & (down < STEPS))
        def _(step=down):
            down_copy(step, got_z).wait_recv()

            @pl.when(q > 0)
            def _():
                down_copy(step, got_z).start()

            @pl.when(step < 4)
            def _():
                relay_copy(step + 4, down_part(step)).start()

        if tick in A_TICKS:
            waiting.pop(0).start()

    def sums(row, count, tiles, base):
        def one(s, carry):
            item = table[row, s]
            column = pl.ds(pl.multiple_of(s * BLK, BLK), BLK)
            first = jnp.where(item < 256, 1.0, 0.0).astype(BF)
            second = jnp.where(item < 256, 0.0, 1.0).astype(BF)
            for which in range(2):
                tile = tiles[base + s, which]
                lhs[which, pl.ds(0, BLK), column] = tile * first
                lhs[which, pl.ds(BLK, BLK), column] = tile * second
            block = item & 31
            rhs[0, column, :] = cells[block // 16, (block // 4) % 4, block % 4]
            rhs[1, column, :] = cot[block // 16, (block // 4) % 4, block % 4]
            return carry

        lax.fori_loop(0, count, one, 0)
        depth = count * BLK
        return [
            jnp.dot(
                lhs[which, :, pl.ds(0, depth)],
                rhs[which, pl.ds(0, depth), :],
                preferred_element_type=F32,
            )
            for which in range(2)
        ]

    for load in loads[1:3]:
        load.wait()
    for share in shares:
        share.wait_recv()

    part_to = [at_chip(across, q), at_chip(two_from, q), at_chip(beyond, q)]
    part_copies = [
        remote(
            part_send.at[g], part_recv.at[g], part_send_sem.at[g], part_recv_sem.at[g], part_to[g]
        )
        for g in range(3)
    ]

    def send_part(g, row, count, tiles, base):
        result = sums(row, count, tiles, base)
        for which in range(2):
            part_send[g, which] = result[which].astype(BF)
        part_copies[g].start()

    send_part(0, 5, SLOTS, got_z, 16)
    two.wait_recv()
    send_part(1, 6, T2, got_two, 0)
    for step in range(4):
        relay_copy(step, up_part(step)).wait_recv()
        relay_copy(step + 4, down_part(step)).wait_recv()
    send_part(2, 4, SLOTS, got_y, 0)
    pack(3, SLOTS, own_packed, 0)
    result = sums(7, SLOTS, own_packed, 0)
    for which in range(2):
        own_sum[which] = result[which]

    for load in loads[3:5]:
        load.wait()
    for copy in a_copies:
        copy.wait_recv()

    core_copies = [
        remote(
            w_part.at[d, 1 - core],
            core_recv.at[d],
            core_send_sem.at[d],
            core_recv_sem.at[d],
            sibling,
        )
        for d in range(4)
    ]
    order = (1, 2, 3, 0)
    for d in order:
        left = cot_all.at[(x + d) % 4]

        def columns(j, carry, d=d, left=left):
            product = lax.dot_general(
                left[...].reshape(QROWS, CH),
                saved_all[j].reshape(QROWS, CH),
                (((0,), (0,)), ((), ())),
                preferred_element_type=F32,
            )
            span = pl.ds(pl.multiple_of(j * CH, CH), CH)
            for group in range(8):
                for half in range(2):
                    start = (2 * group + half) * 16
                    w_part[d, half, group // 2, pl.ds((group % 2) * 16, 16), span] = product[
                        start : start + 16
                    ]
            return carry

        lax.fori_loop(0, 4, columns, 0)
        core_copies[d].start()

    y_copies = {}
    for d in order:
        core_copies[d].wait_recv()
        for yy in range(4):
            total = w_part[d, core, yy] + core_recv[d, yy]
            y_own[d, yy] = total
            y_send[d, yy] = total.astype(BF)
        for e in range(1, 4):
            y_copies[d, e] = remote(
                y_send.at[d, (y + e) % 4],
                y_recv.at[d, e - 1],
                y_send_sem.at[d, e - 1],
                y_recv_sem.at[d, e - 1],
                along_y[e - 1],
            )
            y_copies[d, e].start()

    for copy in part_copies:
        copy.wait_recv()
    for which in range(2):
        total = own_sum[which]
        for g in range(3):
            total = total + part_recv[g, which].astype(F32)
        agg_all[q, which] = (total * SCALE).astype(BF)
    agg_copies = [
        remote(
            agg_all.at[q], agg_all.at[q], agg_send_sem.at[d], agg_recv_sem.at[d], along_q[d]
        )
        for d in range(3)
    ]
    for copy in agg_copies:
        copy.start()

    x_copies = {}
    for d in order:
        total = y_own[d, y]
        for e in range(1, 4):
            y_copies[d, e].wait_recv()
            total = total + y_recv[d, e - 1].astype(F32)
        if d > 0:
            x_send[d - 1] = total.astype(BF)
            x_copies[d] = remote(
                x_send.at[d - 1],
                x_recv.at[d - 1],
                x_send_sem.at[d - 1],
                x_recv_sem.at[d - 1],
                along_x[d - 1],
            )
            x_copies[d].start()
    for d in range(1, 4):
        x_copies[d].wait_recv()
        total = total + x_recv[d - 1].astype(F32)
    for hh in range(2):
        for qq in range(4):
            z_send[hh, qq] = total[hh * 16 : hh * 16 + 16, qq * CH : qq * CH + CH]
    z_copies = []
    for hd in range(2):
        for qd in range(4):
            if hd + qd > 0:
                index = hd * 4 + qd - 1
                chan = (q + qd) % 4
                device = at_chip(across, chan) if hd else (band, chan)
                to_h = 1 - h if hd else h
                z_copies.append(
                    remote(
                        z_send.at[to_h, chan],
                        z_recv.at[index],
                        z_send_sem.at[index],
                        z_recv_sem.at[index],
                        device,
                    )
                )
    for copy in z_copies:
        copy.start()

    for load in loads[5:8]:
        load.wait()
    for copy in agg_copies:
        copy.wait_recv()
    mixed = jnp.zeros((NODES, CH), F32)
    grad = jnp.zeros((NODES, CH), F32)
    for j in range(4):
        mixed = mixed + jnp.dot(
            agg_all[j, 0], mix[pl.ds(j * CH, CH), :], preferred_element_type=F32
        )
    hidden_out[...] = (embed[...].astype(F32) + mixed / (1.0 + jnp.exp(-mixed))).astype(BF)
    for j in range(4):
        grad = grad + jnp.dot(
            agg_all[j, 1], proj[pl.ds(j * CH, CH), :], preferred_element_type=F32
        )
    grad_out[...] = grad.astype(BF)

    total = z_send[h, q]
    for index, copy in enumerate(z_copies):
        copy.wait_recv()
        total = total + z_recv[index]
    w_out[...] = total * (ROWS * 64) ** (-0.5)

    for step in range(STEPS):
        up_copy(step, got_z).wait_send()
        down_copy(step, got_z).wait_send()
        relay_copy(step, up_part(step % 4)).wait_send()
    two.wait_send()
    ends = shares + a_copies + part_copies + core_copies + agg_copies + z_copies
    for copy in ends + list(y_copies.values()) + list(x_copies.values()):
        copy.wait_send()


def shards(
    cells_next, node_embed, enc_mix, out_cotangent, decoded_saved, dec_proj, tile_source, tile_codes
):
    my_band = lax.axis_index("band")
    table = slot_tables(tile_source, my_band)
    hbm = pl.BlockSpec(memory_space=pl.ANY)
    vmem = pl.BlockSpec(memory_space=pltpu.VMEM)
    dma = pltpu.SemaphoreType.DMA
    scratch = [
        pltpu.VMEM((TILES, BLK, BLK), jnp.int32),
        pltpu.VMEM((2, 4, 4, BLK, CH), BF),
        pltpu.VMEM((2, 4, 4, BLK, CH), BF),
        pltpu.VMEM((4, 4, BLK, CH), BF),
        pltpu.VMEM((4, 4, BLK, CH), BF),
        pltpu.VMEM((4 * CH, CH), BF),
        pltpu.VMEM((4 * CH, CH), BF),
        pltpu.VMEM((NODES, CH), BF),
        pltpu.VMEM((2 * SLOTS + T2, 2, BLK, BLK), BF),
        pltpu.VMEM((SLOTS, 2, BLK, BLK), BF),
        pltpu.VMEM((2 * SLOTS, 2, BLK, BLK), BF),
        pltpu.VMEM((SLOTS, 2, BLK, BLK), BF),
        pltpu.VMEM((T2, 2, BLK, BLK), BF),
        pltpu.VMEM((2, NODES, SLOTS * BLK), BF),
        pltpu.VMEM((2, SLOTS * BLK, CH), BF),
        pltpu.VMEM((2, NODES, CH), F32),
        pltpu.VMEM((3, 2, NODES, CH), BF),
        pltpu.VMEM((3, 2, NODES, CH), BF),
        pltpu.VMEM((4, 2, NODES, CH), BF),
        pltpu.VMEM((4, 2, 4, 32, 4 * CH), F32),
        pltpu.VMEM((4, 4, 32, 4 * CH), F32),
        pltpu.VMEM((4, 4, 32, 4 * CH), F32),
        pltpu.VMEM((4, 4, 32, 4 * CH), BF),
        pltpu.VMEM((4, 3, 32, 4 * CH), BF),
        pltpu.VMEM((3, 32, 4 * CH), BF),
        pltpu.VMEM((3, 32, 4 * CH), BF),
        pltpu.VMEM((2, 4, 16, CH), F32),
        pltpu.VMEM((7, 16, CH), F32),
        dma((8,)),
        dma((2,)),
        dma((2,)),
        dma((8,)),
        dma((8,)),
        dma((8,)),
        dma((8,)),
        dma((8,)),
        dma((8,)),
        dma,
        dma,
        dma((6,)),
        dma((6,)),
        dma((4,)),
        dma((4,)),
        dma((4, 3)),
        dma((4, 3)),
        dma((3,)),
        dma((3,)),
        dma((7,)),
        dma((7,)),
        dma((3,)),
        dma((3,)),
        dma((3,)),
        dma((3,)),
    ]
    hidden_nodes, node_grad, w_dec_grad = pl.pallas_call(
        kernel,
        out_shape=(
            jax.ShapeDtypeStruct((NODES, CH), BF),
            jax.ShapeDtypeStruct((NODES, CH), BF),
            jax.ShapeDtypeStruct((16, CH), F32),
        ),
        in_specs=[pl.BlockSpec(memory_space=pltpu.SMEM)] + [hbm] * 7,
        out_specs=(vmem, vmem, vmem),
        scratch_shapes=scratch,
        compiler_params=pltpu.CompilerParams(
            collective_id=0, has_side_effects=True, vmem_limit_bytes=60 * 1024 * 1024
        ),
        name="encode_and_backward",
    )(
        table,
        cells_next.reshape(4, 4, BLK, CH),
        node_embed,
        enc_mix,
        out_cotangent.reshape(4, 4, BLK, CH),
        decoded_saved.reshape(4, 4, BLK, CH),
        dec_proj,
        tile_codes.reshape(TILES, BLK, BLK),
    )
    return hidden_nodes, node_grad, w_dec_grad


def solution(mesh):
    in_specs = (
        P("band", "chan"),
        P("band", "chan"),
        P(None, "chan"),
        P("band", "chan"),
        P("band", "chan"),
        P(None, "chan"),
        P(),
        P("band", None, None, None),
    )
    out_specs = (P("band", "chan"), P("band", "chan"), P("band", "chan"))
    return jax.shard_map(shards, mesh=mesh, in_specs=in_specs, out_specs=out_specs, check_vma=False)
```

```python
import jax
import jax.numpy as jnp
from jax import lax
from jax.experimental import pallas as pl
from jax.experimental.pallas import tpu as pltpu
from jax.sharding import PartitionSpec as P

BLK = 128
K = 16
NB_DEV = 2
CHIPS = 32
TILES = NB_DEV * K
SLOTS = 16
T2 = 8
CH = 256
ROWS = 2048
QROWS = 512
NODES = 256
SCALE = (3.0 / (K * BLK)) ** 0.5 / 128.0
MESH = pl.DeviceIdType.MESH
BF = jnp.bfloat16
F32 = jnp.float32

CHUNK = 2
STEPS = 10
SHORT = 6
A_FIRST = 4
A_TICKS = (1,1,1,1,1,1,1,1,0,0,0)
TWO_TICK = 5
OWN_TICK = 6
BEYOND_TICK = 8


def chip_links(chip, z_hi, core):
    side = 1 - 2 * z_hi
    across = chip + side
    beyond = (chip - side + CHIPS) % CHIPS
    relay_to = (chip + 2 * side + CHIPS) % CHIPS
    two_to = (chip + 4 * core - 2 + CHIPS) % CHIPS
    two_from = (chip - 4 * core + 2 + CHIPS) % CHIPS
    return across, beyond, relay_to, two_to, two_from


def slot_tables(tile_source, my_band):
    chip, core = my_band // 2, my_band % 2
    across, beyond, _, two_to, two_from = chip_links(chip, chip % 2, core)
    targets = jnp.stack(
        [my_band] * 4 + [2 * beyond + core, 2 * across + core, 2 * two_from + core, my_band]
    )
    sources = jnp.stack([beyond, across, two_to, chip, chip, chip, chip, chip])
    blocks = tile_source.reshape(-1, TILES)[targets]
    tile = jnp.arange(TILES, dtype=jnp.int32)
    match = (blocks // 32) == sources[:, None]
    before = tile[None, :, None] > tile[None, None, :]
    rank = jnp.sum((match[:, None, :] & before).astype(jnp.int32), axis=2)
    sending = (jnp.arange(8) < 4)[:, None]
    entry = jnp.where(sending, tile[None, :] + 256, blocks % 32 + 256 * (tile[None, :] // K))
    slot = jnp.arange(SLOTS, dtype=jnp.int32)
    chosen = match[:, :, None] & (rank[:, :, None] == slot[None, None, :])
    return jnp.sum(jnp.where(chosen, entry[:, :, None], 0), axis=1)


def kernel(
    table,
    cells_hbm,
    embed_hbm,
    mix_hbm,
    cot_hbm,
    saved_hbm,
    proj_hbm,
    codes_hbm,
    hidden_out,
    grad_out,
    w_out,
    codes,
    cells,
    cot,
    cot_all,
    saved_all,
    mix,
    proj,
    embed,
    packed,
    own_packed,
    got_z,
    got_y,
    got_two,
    lhs,
    rhs,
    own_sum,
    side_sum,
    beyond_send,
    beyond_recv,
    part_send,
    part_recv,
    agg_all,
    w_part,
    core_recv,
    y_own,
    y_send,
    y_recv,
    x_send,
    x_recv,
    z_send,
    z_recv,
    load_sem,
    share_send,
    share_recv,
    up_send,
    up_recv,
    down_send,
    down_recv,
    relay_send,
    relay_recv,
    two_send,
    two_recv,
    a_send,
    a_recv,
    core_send_sem,
    core_recv_sem,
    y_send_sem,
    y_recv_sem,
    x_send_sem,
    x_recv_sem,
    z_send_sem,
    z_recv_sem,
    beyond_send_sem,
    beyond_recv_sem,
    part_send_sem,
    part_recv_sem,
    agg_send_sem,
    agg_recv_sem,
    hop_send_sem,
):
    band = lax.axis_index("band")
    q = lax.axis_index("chan")
    core = band % 2
    chip = band // 2
    h = chip % 2
    y = (band // 4) % 4
    x = band // 16
    across, beyond, relay_to, two_to, two_from = chip_links(chip, h, core)

    def at_chip(other_chip, chan):
        return (2 * other_chip + core, chan)

    def remote(src, dst, send, recv, device):
        return pltpu.make_async_remote_copy(
            src_ref=src,
            dst_ref=dst,
            send_sem=send,
            recv_sem=recv,
            device_id=device,
            device_id_type=MESH,
        )

    sibling = (band + 1 - 2 * core, q)
    across_q = [at_chip(across, (q + d) % 4) for d in range(4)]
    along_q = [(band, (q + d) % 4) for d in range(1, 4)]
    along_y = [(x * 16 + ((y + d) % 4) * 4 + h * 2 + core, q) for d in range(1, 4)]
    along_x = [(((x + d) % 4) * 16 + y * 4 + h * 2 + core, q) for d in range(1, 4)]

    barrier = pltpu.get_barrier_semaphore()
    partners = (
        [sibling]
        + across_q
        + along_q
        + along_y
        + along_x
        + [at_chip(two_to, q), at_chip(two_from, q)]
    )
    for partner in partners:
        pl.semaphore_signal(barrier, inc=1, device_id=partner, device_id_type=MESH)

    loads = [
        pltpu.make_async_copy(codes_hbm, codes, load_sem.at[0]),
        pltpu.make_async_copy(cells_hbm, cells.at[core], load_sem.at[1]),
        pltpu.make_async_copy(cot_hbm, cot.at[core], load_sem.at[2]),
        pltpu.make_async_copy(cot_hbm.at[q], cot_all.at[q], load_sem.at[3]),
        pltpu.make_async_copy(saved_hbm.at[q], saved_all.at[q], load_sem.at[4]),
        pltpu.make_async_copy(mix_hbm, mix, load_sem.at[5]),
        pltpu.make_async_copy(proj_hbm, proj, load_sem.at[6]),
        pltpu.make_async_copy(embed_hbm, embed, load_sem.at[7]),
    ]
    for load in loads:
        load.start()

    def pack(row, count, dest, base):
        def one(s, carry):
            item = table[row, s]
            words = codes[item & 31]
            low = ((words & 255) - 128).astype(F32)
            high = ((words >> 8) - 128).astype(F32)
            keep = jnp.where(item >= 256, 1.0, 0.0).astype(F32)
            dest[base + s, 0] = (low * keep).astype(BF)
            dest[base + s, 1] = (high * keep).astype(BF)
            return carry

        lax.fori_loop(0, count, one, 0)

    a_copies = []
    for half in range(2):
        for d in (1, 3, 2):
            other = (q + d) % 4
            for array, (src, dst) in enumerate(((cot_hbm, cot_all), (saved_hbm, saved_all))):
                index = 2 * (d - 1) + array
                part = pl.ds(2 * half, 2)
                a_copies.append(
                    remote(
                        src.at[other, part],
                        dst.at[q, part],
                        a_send.at[half, index],
                        a_recv.at[half, index],
                        (band, other),
                    )
                )
    waiting = list(a_copies)

    pl.semaphore_wait(barrier, len(partners))
    for _ in range(A_FIRST):
        waiting.pop(0).start()
    loads[0].wait()
    pack(0, SLOTS, packed, 0)
    pack(1, SLOTS, packed, 16)
    pack(2, T2, packed, 32)

    z_up = at_chip(jnp.where(q == 3, across, chip), (q + 1) % 4)
    z_down = at_chip(jnp.where(q == 0, across, chip), (q + 3) % 4)

    def up_part(step):
        return pl.ds(CHUNK * step + 8 * (step // 4) - 4 * (step // 8), CHUNK)

    def down_part(step):
        return pl.ds(CHUNK * step + 8 + 8 * (step // 4) - 20 * (step // 8), CHUNK)

    def up_copy(step, src):
        part = up_part(step)
        return remote(src.at[part], got_z.at[part], up_send.at[step], up_recv.at[step], z_up)

    def down_copy(step, src):
        part = down_part(step)
        return remote(src.at[part], got_z.at[part], down_send.at[step], down_recv.at[step], z_down)

    def relay_copy(index, part):
        return remote(
            got_z.at[part],
            got_y.at[part],
            relay_send.at[index],
            relay_recv.at[index],
            at_chip(relay_to, q),
        )

    for step in range(STEPS):

        @pl.when(q == 3)
        def _(step=step):
            up_copy(step, packed).start()

        @pl.when(q == 0)
        def _(step=step):
            down_copy(step, packed).start()

    two = remote(packed.at[pl.ds(32, T2)], got_two, two_send, two_recv, at_chip(two_to, q))
    two.start()
    shares = [
        remote(cells_hbm, cells.at[core], share_send.at[0], share_recv.at[0], sibling),
        remote(cot_hbm, cot.at[core], share_send.at[1], share_recv.at[1], sibling),
    ]
    for share in shares:
        share.start()

    def sums(row, count, tiles, base):
        def one(s, carry):
            item = table[row, s]
            column = pl.ds(pl.multiple_of(s * BLK, BLK), BLK)
            first = jnp.where(item < 256, 1.0, 0.0).astype(BF)
            second = jnp.where(item < 256, 0.0, 1.0).astype(BF)
            for which in range(2):
                tile = tiles[base + s, which]
                lhs[which, pl.ds(0, BLK), column] = tile * first
                lhs[which, pl.ds(BLK, BLK), column] = tile * second
            block = item & 31
            rhs[0, column, :] = cells[block // 16, (block // 4) % 4, block % 4]
            rhs[1, column, :] = cot[block // 16, (block // 4) % 4, block % 4]
            return carry

        lax.fori_loop(0, count, one, 0)
        depth = count * BLK
        return [
            jnp.dot(
                lhs[which, :, pl.ds(0, depth)],
                rhs[which, pl.ds(0, depth), :],
                preferred_element_type=F32,
            )
            for which in range(2)
        ]

    beyond_copies = [
        remote(
            beyond_send.at[which],
            beyond_recv.at[which],
            beyond_send_sem.at[which],
            beyond_recv_sem.at[which],
            at_chip((chip - 2 * (1 - 2 * h) + CHIPS) % CHIPS, q),
        )
        for which in range(2)
    ]

    def send_beyond():
        for step in range(4):
            relay_copy(step, up_part(step)).wait_recv()
            relay_copy(step + 4, down_part(step)).wait_recv()
        result = sums(4, SLOTS, got_y, 0)
        for which in range(2):
            beyond_send[which] = result[which].astype(BF)
            beyond_copies[which].start()

    part_copies = [
        [
            remote(
                part_send.at[g, which],
                part_recv.at[g, which],
                part_send_sem.at[g, which],
                part_recv_sem.at[g, which],
                at_chip(to, q),
            )
            for which in range(2)
        ]
        for g, to in enumerate((across, two_from))
    ]

    def send_two():
        two.wait_recv()
        result = sums(6, T2, got_two, 0)
        for which in range(2):
            part_send[1, which] = result[which].astype(BF)
            part_copies[1][which].start()

    def sum_own():
        pack(3, SLOTS, own_packed, 0)
        result = sums(7, SLOTS, own_packed, 0)
        for which in range(2):
            own_sum[which] = result[which]

    for tick in range(STEPS + 1):
        if tick == TWO_TICK:
            for load in loads[1:3]:
                load.wait()
            for share in shares:
                share.wait_recv()
            send_two()
        if tick == OWN_TICK:
            sum_own()
        if tick == BEYOND_TICK:
            send_beyond()
        up, down = tick - q, tick - 3 + q

        @pl.when((up >= 0) & (up < STEPS) & ((up < SHORT) | (q < 2)))
        def _(step=up):
            up_copy(step, got_z).wait_recv()

            @pl.when((q < 3) & ((step < SHORT) | (q < 1)))
            def _():
                up_copy(step, got_z).start()

            @pl.when(step < 4)
            def _():
                relay_copy(step, up_part(step)).start()

        @pl.when((down >= 0) & (down < STEPS) & ((down < SHORT) | (q > 1)))
        def _(step=down):
            down_copy(step, got_z).wait_recv()

            @pl.when((q > 0) & ((step < SHORT) | (q > 2)))
            def _():
                down_copy(step, got_z).start()

            @pl.when(step < 4)
            def _():
                relay_copy(step + 4, down_part(step)).start()

        for _ in range(A_TICKS[tick]):
            waiting.pop(0).start()

    result = sums(5, SLOTS, got_z, 16)
    for which in range(2):
        side_sum[which] = result[which]
    for which in range(2):
        beyond_copies[which].wait_recv()
        total = side_sum[which] + beyond_recv[which].astype(F32)
        part_send[0, which] = total.astype(BF)
        part_copies[0][which].start()
    for copy in waiting:
        copy.start()

    for load in loads[3:5]:
        load.wait()
    for copy in a_copies:
        copy.wait_recv()

    core_copies = [
        remote(
            w_part.at[d, 1 - core],
            core_recv.at[d],
            core_send_sem.at[d],
            core_recv_sem.at[d],
            sibling,
        )
        for d in range(4)
    ]
    order = (1, 2, 3, 0)
    for d in order:
        left = cot_all.at[(x + d) % 4]

        def columns(j, carry, d=d, left=left):
            product = lax.dot_general(
                left[...].reshape(QROWS, CH),
                saved_all[j].reshape(QROWS, CH),
                (((0,), (0,)), ((), ())),
                preferred_element_type=F32,
            )
            span = pl.ds(pl.multiple_of(j * CH, CH), CH)
            for group in range(8):
                for half in range(2):
                    start = (2 * group + half) * 16
                    w_part[d, half, group // 2, pl.ds((group % 2) * 16, 16), span] = product[
                        start : start + 16
                    ]
            return carry

        lax.fori_loop(0, 4, columns, 0)
        core_copies[d].start()

    y_copies = {}
    for d in order:
        core_copies[d].wait_recv()
        for yy in range(4):
            total = w_part[d, core, yy] + core_recv[d, yy]
            y_own[d, yy] = total
            y_send[d, yy] = total.astype(BF)
        for e in range(1, 4):
            y_copies[d, e] = remote(
                y_send.at[d, (y + e) % 4],
                y_recv.at[d, e - 1],
                y_send_sem.at[d, e - 1],
                y_recv_sem.at[d, e - 1],
                along_y[e - 1],
            )
            y_copies[d, e].start()

    def agg_copy(d, which):
        return remote(
            agg_all.at[q, which],
            agg_all.at[q, which],
            agg_send_sem.at[d - 1, which],
            agg_recv_sem.at[d - 1, which],
            (band, (q + d) % 4),
        )

    def hop_copy(which):
        block = (q + 2) % 4
        return remote(
            agg_all.at[block, which],
            agg_all.at[block, which],
            hop_send_sem.at[which],
            agg_recv_sem.at[2 * (q - 1), which],
            (band, 3 * (q - 1)),
        )

    middle = (q == 1) | (q == 2)

    def far(d):
        return ((q == 0) & (d == 3)) | ((q == 3) & (d == 1))

    for which in range(2):
        total = own_sum[which]
        for g in range(2):
            part_copies[g][which].wait_recv()
            total = total + part_recv[g, which].astype(F32)
        agg_all[q, which] = (total * SCALE).astype(BF)
        for d in (2, 1, 3):

            @pl.when(jnp.logical_not(far(d)))
            def _(d=d, which=which):
                agg_copy(d, which).start()

    x_copies = {}
    for d in order:
        total = y_own[d, y]
        for e in range(1, 4):
            y_copies[d, e].wait_recv()
            total = total + y_recv[d, e - 1].astype(F32)
        if d > 0:
            x_send[d - 1] = total.astype(BF)
            x_copies[d] = remote(
                x_send.at[d - 1],
                x_recv.at[d - 1],
                x_send_sem.at[d - 1],
                x_recv_sem.at[d - 1],
                along_x[d - 1],
            )
            x_copies[d].start()
    for which in range(2):
        agg_copy(2, which).wait_recv()

        @pl.when(middle)
        def _(which=which):
            hop_copy(which).start()

    for d in range(1, 4):
        x_copies[d].wait_recv()
        total = total + x_recv[d - 1].astype(F32)
    for hh in range(2):
        for qq in range(4):
            z_send[hh, qq] = total[hh * 16 : hh * 16 + 16, qq * CH : qq * CH + CH]
    z_copies = []
    for hd in range(2):
        for qd in range(4):
            if hd + qd > 0:
                index = hd * 4 + qd - 1
                chan = (q + qd) % 4
                device = at_chip(across, chan) if hd else (band, chan)
                to_h = 1 - h if hd else h
                z_copies.append(
                    remote(
                        z_send.at[to_h, chan],
                        z_recv.at[index],
                        z_send_sem.at[index],
                        z_recv_sem.at[index],
                        device,
                    )
                )
    for copy in z_copies:
        copy.start()

    for load in loads[5:8]:
        load.wait()
    for d in (1, 3):
        agg_copy(d, 0).wait_recv()
    mixed = jnp.zeros((NODES, CH), F32)
    grad = jnp.zeros((NODES, CH), F32)
    for j in range(4):
        mixed = mixed + jnp.dot(
            agg_all[j, 0], mix[pl.ds(j * CH, CH), :], preferred_element_type=F32
        )
    hidden_out[...] = (embed[...].astype(F32) + mixed / (1.0 + jnp.exp(-mixed))).astype(BF)
    for d in (1, 3):
        agg_copy(d, 1).wait_recv()
    for j in range(4):
        grad = grad + jnp.dot(
            agg_all[j, 1], proj[pl.ds(j * CH, CH), :], preferred_element_type=F32
        )
    grad_out[...] = grad.astype(BF)

    total = z_send[h, q]
    for index, copy in enumerate(z_copies):
        copy.wait_recv()
        total = total + z_recv[index]
    w_out[...] = total * (ROWS * 64) ** (-0.5)

    for step in range(STEPS):

        @pl.when((q == 0) | (q == 3) | (step < SHORT))
        def _(step=step):
            up_copy(step, got_z).wait_send()
            down_copy(step, got_z).wait_send()

    for step in range(4):
        relay_copy(step, up_part(step)).wait_send()
        relay_copy(step + 4, down_part(step)).wait_send()
    two.wait_send()
    for which in range(2):
        for d in range(1, 4):

            @pl.when(jnp.logical_not(far(d)))
            def _(d=d, which=which):
                agg_copy(d, which).wait_send()

        @pl.when(middle)
        def _(which=which):
            hop_copy(which).wait_send()

    ends = shares + a_copies + beyond_copies + part_copies[0] + part_copies[1]
    ends = ends + core_copies + z_copies
    for copy in ends + list(y_copies.values()) + list(x_copies.values()):
        copy.wait_send()


def shards(
    cells_next, node_embed, enc_mix, out_cotangent, decoded_saved, dec_proj, tile_source, tile_codes
):
    my_band = lax.axis_index("band")
    table = slot_tables(tile_source, my_band)
    hbm = pl.BlockSpec(memory_space=pl.ANY)
    vmem = pl.BlockSpec(memory_space=pltpu.VMEM)
    dma = pltpu.SemaphoreType.DMA
    scratch = [
        pltpu.VMEM((TILES, BLK, BLK), jnp.int32),
        pltpu.VMEM((2, 4, 4, BLK, CH), BF),
        pltpu.VMEM((2, 4, 4, BLK, CH), BF),
        pltpu.VMEM((4, 4, BLK, CH), BF),
        pltpu.VMEM((4, 4, BLK, CH), BF),
        pltpu.VMEM((4 * CH, CH), BF),
        pltpu.VMEM((4 * CH, CH), BF),
        pltpu.VMEM((NODES, CH), BF),
        pltpu.VMEM((2 * SLOTS + T2, 2, BLK, BLK), BF),
        pltpu.VMEM((SLOTS, 2, BLK, BLK), BF),
        pltpu.VMEM((2 * SLOTS, 2, BLK, BLK), BF),
        pltpu.VMEM((SLOTS, 2, BLK, BLK), BF),
        pltpu.VMEM((T2, 2, BLK, BLK), BF),
        pltpu.VMEM((2, NODES, SLOTS * BLK), BF),
        pltpu.VMEM((2, SLOTS * BLK, CH), BF),
        pltpu.VMEM((2, NODES, CH), F32),
        pltpu.VMEM((2, NODES, CH), F32),
        pltpu.VMEM((2, NODES, CH), BF),
        pltpu.VMEM((2, NODES, CH), BF),
        pltpu.VMEM((2, 2, NODES, CH), BF),
        pltpu.VMEM((2, 2, NODES, CH), BF),
        pltpu.VMEM((4, 2, NODES, CH), BF),
        pltpu.VMEM((4, 2, 4, 32, 4 * CH), F32),
        pltpu.VMEM((4, 4, 32, 4 * CH), F32),
        pltpu.VMEM((4, 4, 32, 4 * CH), F32),
        pltpu.VMEM((4, 4, 32, 4 * CH), BF),
        pltpu.VMEM((4, 3, 32, 4 * CH), BF),
        pltpu.VMEM((3, 32, 4 * CH), BF),
        pltpu.VMEM((3, 32, 4 * CH), BF),
        pltpu.VMEM((2, 4, 16, CH), F32),
        pltpu.VMEM((7, 16, CH), F32),
        dma((8,)),
        dma((2,)),
        dma((2,)),
        dma((10,)),
        dma((10,)),
        dma((10,)),
        dma((10,)),
        dma((8,)),
        dma((8,)),
        dma,
        dma,
        dma((2, 6)),
        dma((2, 6)),
        dma((4,)),
        dma((4,)),
        dma((4, 3)),
        dma((4, 3)),
        dma((3,)),
        dma((3,)),
        dma((7,)),
        dma((7,)),
        dma((2,)),
        dma((2,)),
        dma((2, 2)),
        dma((2, 2)),
        dma((3, 2)),
        dma((3, 2)),
        dma((2,)),
    ]
    hidden_nodes, node_grad, w_dec_grad = pl.pallas_call(
        kernel,
        out_shape=(
            jax.ShapeDtypeStruct((NODES, CH), BF),
            jax.ShapeDtypeStruct((NODES, CH), BF),
            jax.ShapeDtypeStruct((16, CH), F32),
        ),
        in_specs=[pl.BlockSpec(memory_space=pltpu.SMEM)] + [hbm] * 7,
        out_specs=(vmem, vmem, vmem),
        scratch_shapes=scratch,
        compiler_params=pltpu.CompilerParams(
            collective_id=0, has_side_effects=True, vmem_limit_bytes=60 * 1024 * 1024
        ),
        name="encode_and_backward",
    )(
        table,
        cells_next.reshape(4, 4, BLK, CH),
        node_embed,
        enc_mix,
        out_cotangent.reshape(4, 4, BLK, CH),
        decoded_saved.reshape(4, 4, BLK, CH),
        dec_proj,
        tile_codes.reshape(TILES, BLK, BLK),
    )
    return hidden_nodes, node_grad, w_dec_grad


def solution(mesh):
    in_specs = (
        P("band", "chan"),
        P("band", "chan"),
        P(None, "chan"),
        P("band", "chan"),
        P("band", "chan"),
        P(None, "chan"),
        P(),
        P("band", None, None, None),
    )
    out_specs = (P("band", "chan"), P("band", "chan"), P("band", "chan"))
    return jax.shard_map(shards, mesh=mesh, in_specs=in_specs, out_specs=out_specs, check_vma=False)
```

```python
import jax
import jax.numpy as jnp
from jax import lax
from jax.experimental import pallas as pl
from jax.experimental.pallas import tpu as pltpu
from jax.sharding import PartitionSpec as P

BLK = 128
K = 16
NB_DEV = 2
CHIPS = 32
TILES = NB_DEV * K
SLOTS = 16
T2 = 8
CH = 256
ROWS = 2048
QROWS = 512
NODES = 256
SCALE = (3.0 / (K * BLK)) ** 0.5 / 128.0
MESH = pl.DeviceIdType.MESH
BF = jnp.bfloat16
F32 = jnp.float32

Z_SLOTS = 24
CHUNK = 2
STEPS = 8
SHORT = 4
A_FIRST = 4
A_TICKS = (1, 1, 1, 1, 1, 1, 1, 1, 0)
TWO_TICK = 4
OWN_TICK = 5
BEYOND_TICK = 7


def chip_links(chip, z_hi, core):
    side = 1 - 2 * z_hi
    across = chip + side
    beyond = (chip - side + CHIPS) % CHIPS
    relay_to = (chip + 2 * side + CHIPS) % CHIPS
    two_to = (chip + 4 * core - 2 + CHIPS) % CHIPS
    two_from = (chip - 4 * core + 2 + CHIPS) % CHIPS
    return across, beyond, relay_to, two_to, two_from


def kernel(
    source,
    cells_hbm,
    embed_hbm,
    mix_hbm,
    cot_hbm,
    saved_hbm,
    proj_hbm,
    codes_hbm,
    hidden_out,
    grad_out,
    w_out,
    table,
    table_rows,
    codes,
    cells,
    cot,
    cot_all,
    saved_all,
    mix,
    proj,
    embed,
    packed,
    own_packed,
    got_z,
    got_y,
    got_two,
    lhs,
    rhs,
    own_sum,
    side_sum,
    beyond_send,
    beyond_recv,
    part_send,
    part_recv,
    agg_all,
    w_part,
    core_recv,
    y_own,
    y_send,
    y_recv,
    x_send,
    x_recv,
    z_send,
    z_recv,
    load_sem,
    share_send,
    share_recv,
    up_send,
    up_recv,
    down_send,
    down_recv,
    relay_send,
    relay_recv,
    two_send,
    two_recv,
    a_send,
    a_recv,
    core_send_sem,
    core_recv_sem,
    y_send_sem,
    y_recv_sem,
    x_send_sem,
    x_recv_sem,
    z_send_sem,
    z_recv_sem,
    beyond_send_sem,
    beyond_recv_sem,
    part_send_sem,
    part_recv_sem,
    agg_send_sem,
    agg_recv_sem,
    hop_send_sem,
):
    band = lax.axis_index("band")
    q = lax.axis_index("chan")
    core = band % 2
    chip = band // 2
    h = chip % 2
    y = (band // 4) % 4
    x = band // 16
    across, beyond, relay_to, two_to, two_from = chip_links(chip, h, core)

    def at_chip(other_chip, chan):
        return (2 * other_chip + core, chan)

    def remote(src, dst, send, recv, device):
        return pltpu.make_async_remote_copy(
            src_ref=src,
            dst_ref=dst,
            send_sem=send,
            recv_sem=recv,
            device_id=device,
            device_id_type=MESH,
        )

    sibling = (band + 1 - 2 * core, q)
    across_q = [at_chip(across, (q + d) % 4) for d in range(4)]
    along_q = [(band, (q + d) % 4) for d in range(1, 4)]
    along_y = [(x * 16 + ((y + d) % 4) * 4 + h * 2 + core, q) for d in range(1, 4)]
    along_x = [(((x + d) % 4) * 16 + y * 4 + h * 2 + core, q) for d in range(1, 4)]

    barrier = pltpu.get_barrier_semaphore()
    partners = (
        [sibling]
        + across_q
        + along_q
        + along_y
        + along_x
        + [at_chip(two_to, q), at_chip(two_from, q)]
    )
    for partner in partners:
        pl.semaphore_signal(barrier, inc=1, device_id=partner, device_id_type=MESH)

    loads = [
        pltpu.make_async_copy(codes_hbm, codes, load_sem.at[0]),
        pltpu.make_async_copy(cells_hbm, cells.at[core], load_sem.at[1]),
        pltpu.make_async_copy(cot_hbm, cot.at[core], load_sem.at[2]),
        pltpu.make_async_copy(cot_hbm.at[q], cot_all.at[q], load_sem.at[3]),
        pltpu.make_async_copy(saved_hbm.at[q], saved_all.at[q], load_sem.at[4]),
        pltpu.make_async_copy(mix_hbm, mix, load_sem.at[5]),
        pltpu.make_async_copy(proj_hbm, proj, load_sem.at[6]),
        pltpu.make_async_copy(embed_hbm, embed, load_sem.at[7]),
    ]
    for load in loads:
        load.start()

    lane = lax.broadcasted_iota(jnp.int32, (8, BLK), 1)
    row = lax.broadcasted_iota(jnp.int32, (8, BLK), 0)

    def place(t, carry):
        rows, ranks = carry
        own, far, near, two = (
            source[t % K, 2 * owner + t // K]
            for owner in (band, 2 * beyond + core, 2 * across + core, 2 * two_from + core)
        )
        hits = (
            own // 32 == beyond,
            own // 32 == across,
            own // 32 == two_to,
            own // 32 == chip,
            far // 32 == chip,
            near // 32 == chip,
            two // 32 == chip,
        )
        half = 256 * (t // K) + 512
        entries = (
            (0, hits[0], ranks[0], t + 256),
            (0, hits[1], Z_SLOTS - 1 - ranks[1], t + 256),
            (2, hits[2], ranks[2], t + 256),
            (3, hits[3], ranks[3], t + 256),
            (4, hits[4], ranks[4], far % 32 + half + 1024 * ranks[4]),
            (5, hits[5], ranks[5], near % 32 + half + 1024 * (Z_SLOTS - 1 - ranks[5])),
            (6, hits[6], ranks[6], two % 32 + half + 1024 * ranks[6]),
            (7, hits[3], ranks[3], own % 32 + half + 1024 * ranks[3]),
        )
        for index, hit, slot, value in entries:
            spot = (row == index) & (lane == jnp.where(hit, slot, -1))
            rows = jnp.where(spot, value, rows)
        ranks = tuple(rank + jnp.where(hit, 1, 0) for rank, hit in zip(ranks, hits))
        return rows, ranks

    zero = jnp.int32(0)
    table_rows[...] = lax.fori_loop(
        0, TILES, place, (jnp.zeros((8, BLK), jnp.int32), (zero,) * 7)
    )[0]
    table_load = pltpu.make_async_copy(table_rows, table, load_sem.at[8])

    def pack(row, count, dest, base):
        def one(s, carry):
            item = table[row, s]
            words = codes[item & 31]
            low = ((words & 255) - 128).astype(F32)
            high = ((words >> 8) - 128).astype(F32)
            keep = jnp.where(item >= 256, 1.0, 0.0).astype(F32)
            dest[base + s, 0] = (low * keep).astype(BF)
            dest[base + s, 1] = (high * keep).astype(BF)
            return carry

        lax.fori_loop(0, count, one, 0)

    a_copies = []
    for half in range(2):
        for d in (1, 3, 2):
            other = (q + d) % 4
            for array, (src, dst) in enumerate(((cot_hbm, cot_all), (saved_hbm, saved_all))):
                index = 2 * (d - 1) + array
                part = pl.ds(2 * half, 2)
                a_copies.append(
                    remote(
                        src.at[other, part],
                        dst.at[q, part],
                        a_send.at[half, index],
                        a_recv.at[half, index],
                        (band, other),
                    )
                )
    waiting = list(a_copies)

    pl.semaphore_wait(barrier, len(partners))
    for _ in range(A_FIRST):
        waiting.pop(0).start()
    table_load.start()
    loads[0].wait()
    table_load.wait()
    pack(0, Z_SLOTS, packed, 0)
    pack(2, T2, packed, Z_SLOTS)

    z_up = at_chip(jnp.where(q == 3, across, chip), (q + 1) % 4)
    z_down = at_chip(jnp.where(q == 0, across, chip), (q + 3) % 4)

    def up_part(step):
        return pl.ds(CHUNK * step + 8 * (step // SHORT), CHUNK)

    def down_part(step):
        return pl.ds(CHUNK * step + 8, CHUNK)

    def up_copy(step, src):
        part = up_part(step)
        return remote(src.at[part], got_z.at[part], up_send.at[step], up_recv.at[step], z_up)

    def down_copy(step, src):
        part = down_part(step)
        return remote(src.at[part], got_z.at[part], down_send.at[step], down_recv.at[step], z_down)

    def relay_copy(index, part):
        return remote(
            got_z.at[part],
            got_y.at[part],
            relay_send.at[index],
            relay_recv.at[index],
            at_chip(relay_to, q),
        )

    for step in range(STEPS):

        @pl.when(q == 3)
        def _(step=step):
            up_copy(step, packed).start()

        @pl.when(q == 0)
        def _(step=step):
            down_copy(step, packed).start()

    two = remote(packed.at[pl.ds(Z_SLOTS, T2)], got_two, two_send, two_recv, at_chip(two_to, q))
    two.start()
    shares = [
        remote(cells_hbm, cells.at[core], share_send.at[0], share_recv.at[0], sibling),
        remote(cot_hbm, cot.at[core], share_send.at[1], share_recv.at[1], sibling),
    ]
    for share in shares:
        share.start()

    def sums(row, count, tiles):
        def one(s, carry):
            item = table[row, s]
            column = pl.ds(pl.multiple_of(s * BLK, BLK), BLK)
            first = jnp.where((item & 768) == 512, 1.0, 0.0).astype(BF)
            second = jnp.where((item & 768) == 768, 1.0, 0.0).astype(BF)
            for which in range(2):
                tile = tiles[item // 1024, which]
                lhs[which, pl.ds(0, BLK), column] = tile * first
                lhs[which, pl.ds(BLK, BLK), column] = tile * second
            block = item & 31
            rhs[0, column, :] = cells[block // 16, (block // 4) % 4, block % 4]
            rhs[1, column, :] = cot[block // 16, (block // 4) % 4, block % 4]
            return carry

        lax.fori_loop(0, count, one, 0)
        depth = count * BLK
        return [
            jnp.dot(
                lhs[which, :, pl.ds(0, depth)],
                rhs[which, pl.ds(0, depth), :],
                preferred_element_type=F32,
            )
            for which in range(2)
        ]

    beyond_copies = [
        remote(
            beyond_send.at[which],
            beyond_recv.at[which],
            beyond_send_sem.at[which],
            beyond_recv_sem.at[which],
            at_chip((chip - 2 * (1 - 2 * h) + CHIPS) % CHIPS, q),
        )
        for which in range(2)
    ]

    def send_beyond():
        for step in range(4):
            relay_copy(step, up_part(step)).wait_recv()
            relay_copy(step + 4, down_part(step)).wait_recv()
        result = sums(4, SLOTS, got_y)
        for which in range(2):
            beyond_send[which] = result[which].astype(BF)
            beyond_copies[which].start()

    part_copies = [
        [
            remote(
                part_send.at[g, which],
                part_recv.at[g, which],
                part_send_sem.at[g, which],
                part_recv_sem.at[g, which],
                at_chip(to, q),
            )
            for which in range(2)
        ]
        for g, to in enumerate((across, two_from))
    ]

    def send_two():
        two.wait_recv()
        result = sums(6, T2, got_two)
        for which in range(2):
            part_send[1, which] = result[which].astype(BF)
            part_copies[1][which].start()

    def sum_own():
        pack(3, SLOTS, own_packed, 0)
        result = sums(7, SLOTS, own_packed)
        for which in range(2):
            own_sum[which] = result[which]

    core_copies = [
        remote(
            w_part.at[d, 1 - core],
            core_recv.at[d],
            core_send_sem.at[d],
            core_recv_sem.at[d],
            sibling,
        )
        for d in range(4)
    ]
    order = (1, 2, 3, 0)

    def start_projection():
        for load in loads[3:5]:
            load.wait()
        for copy in a_copies:
            copy.wait_recv()

        for d in order:
            left = cot_all.at[(x + d) % 4]

            def columns(j, carry, d=d, left=left):
                product = lax.dot_general(
                    left[...].reshape(QROWS, CH),
                    saved_all[j].reshape(QROWS, CH),
                    (((0,), (0,)), ((), ())),
                    preferred_element_type=F32,
                )
                span = pl.ds(pl.multiple_of(j * CH, CH), CH)
                for group in range(8):
                    for half in range(2):
                        start = (2 * group + half) * 16
                        w_part[d, half, group // 2, pl.ds((group % 2) * 16, 16), span] = product[
                            start : start + 16
                        ]
                return carry

            lax.fori_loop(0, 4, columns, 0)
            core_copies[d].start()

    for tick in range(STEPS + 1):
        if tick == TWO_TICK:
            for load in loads[1:3]:
                load.wait()
            for share in shares:
                share.wait_recv()
            send_two()
        if tick == OWN_TICK:
            sum_own()
        if tick == BEYOND_TICK:
            send_beyond()
        up, down = tick - q, tick - 3 + q

        @pl.when((up >= 0) & (up < STEPS) & ((up < SHORT) | (q < 2)))
        def _(step=up):
            up_copy(step, got_z).wait_recv()

            @pl.when((q < 3) & ((step < SHORT) | (q < 1)))
            def _():
                up_copy(step, got_z).start()

            @pl.when(step < 4)
            def _():
                relay_copy(step, up_part(step)).start()

        @pl.when((down >= 0) & (down < STEPS) & ((down < SHORT) | (q > 1)))
        def _(step=down):
            down_copy(step, got_z).wait_recv()

            @pl.when((q > 0) & ((step < SHORT) | (q > 2)))
            def _():
                down_copy(step, got_z).start()

            @pl.when(step < 4)
            def _():
                relay_copy(step + 4, down_part(step)).start()

        for _ in range(A_TICKS[tick]):
            waiting.pop(0).start()

    result = sums(5, SLOTS, got_z)
    for which in range(2):
        side_sum[which] = result[which]
    for which in range(2):
        beyond_copies[which].wait_recv()
        total = side_sum[which] + beyond_recv[which].astype(F32)
        part_send[0, which] = total.astype(BF)
        part_copies[0][which].start()
    for copy in waiting:
        copy.start()
    start_projection()

    y_copies = {}
    for d in order:
        core_copies[d].wait_recv()
        for yy in range(4):
            total = w_part[d, core, yy] + core_recv[d, yy]
            y_own[d, yy] = total
            y_send[d, yy] = total.astype(BF)
        for e in range(1, 4):
            y_copies[d, e] = remote(
                y_send.at[d, (y + e) % 4],
                y_recv.at[d, e - 1],
                y_send_sem.at[d, e - 1],
                y_recv_sem.at[d, e - 1],
                along_y[e - 1],
            )
            y_copies[d, e].start()

    def agg_copy(d, which):
        return remote(
            agg_all.at[q, which],
            agg_all.at[q, which],
            agg_send_sem.at[d - 1, which],
            agg_recv_sem.at[d - 1, which],
            (band, (q + d) % 4),
        )

    def hop_copy(which):
        block = (q + 2) % 4
        return remote(
            agg_all.at[block, which],
            agg_all.at[block, which],
            hop_send_sem.at[which],
            agg_recv_sem.at[2 * (q - 1), which],
            (band, 3 * (q - 1)),
        )

    middle = (q == 1) | (q == 2)

    def far(d):
        return ((q == 0) & (d == 3)) | ((q == 3) & (d == 1))

    for which in range(2):
        total = own_sum[which]
        for g in range(2):
            part_copies[g][which].wait_recv()
            total = total + part_recv[g, which].astype(F32)
        agg_all[q, which] = (total * SCALE).astype(BF)
        for d in (2, 1, 3):

            @pl.when(jnp.logical_not(far(d)))
            def _(d=d, which=which):
                agg_copy(d, which).start()

    x_copies = {}
    for d in order:
        total = y_own[d, y]
        for e in range(1, 4):
            y_copies[d, e].wait_recv()
            total = total + y_recv[d, e - 1].astype(F32)
        if d > 0:
            x_send[d - 1] = total.astype(BF)
            x_copies[d] = remote(
                x_send.at[d - 1],
                x_recv.at[d - 1],
                x_send_sem.at[d - 1],
                x_recv_sem.at[d - 1],
                along_x[d - 1],
            )
            x_copies[d].start()
    for which in range(2):
        agg_copy(2, which).wait_recv()

        @pl.when(middle)
        def _(which=which):
            hop_copy(which).start()

    for d in range(1, 4):
        x_copies[d].wait_recv()
        total = total + x_recv[d - 1].astype(F32)
    for hh in range(2):
        for qq in range(4):
            z_send[hh, qq] = total[hh * 16 : hh * 16 + 16, qq * CH : qq * CH + CH]
    z_copies = []
    for hd in range(2):
        for qd in range(4):
            if hd + qd > 0:
                index = hd * 4 + qd - 1
                chan = (q + qd) % 4
                device = at_chip(across, chan) if hd else (band, chan)
                to_h = 1 - h if hd else h
                z_copies.append(
                    remote(
                        z_send.at[to_h, chan],
                        z_recv.at[index],
                        z_send_sem.at[index],
                        z_recv_sem.at[index],
                        device,
                    )
                )
    for copy in z_copies:
        copy.start()

    for load in loads[5:8]:
        load.wait()
    for d in (1, 3):
        agg_copy(d, 0).wait_recv()
    mixed = jnp.zeros((NODES, CH), F32)
    grad = jnp.zeros((NODES, CH), F32)
    for j in range(4):
        mixed = mixed + jnp.dot(
            agg_all[j, 0], mix[pl.ds(j * CH, CH), :], preferred_element_type=F32
        )
    hidden_out[...] = (embed[...].astype(F32) + mixed / (1.0 + jnp.exp(-mixed))).astype(BF)
    for d in (1, 3):
        agg_copy(d, 1).wait_recv()
    for j in range(4):
        grad = grad + jnp.dot(
            agg_all[j, 1], proj[pl.ds(j * CH, CH), :], preferred_element_type=F32
        )
    grad_out[...] = grad.astype(BF)

    total = z_send[h, q]
    for index, copy in enumerate(z_copies):
        copy.wait_recv()
        total = total + z_recv[index]
    w_out[...] = total * (ROWS * 64) ** (-0.5)

    for step in range(STEPS):

        @pl.when((q == 0) | (q == 3) | (step < SHORT))
        def _(step=step):
            up_copy(step, got_z).wait_send()
            down_copy(step, got_z).wait_send()

    for step in range(4):
        relay_copy(step, up_part(step)).wait_send()
        relay_copy(step + 4, down_part(step)).wait_send()
    two.wait_send()
    for which in range(2):
        for d in range(1, 4):

            @pl.when(jnp.logical_not(far(d)))
            def _(d=d, which=which):
                agg_copy(d, which).wait_send()

        @pl.when(middle)
        def _(which=which):
            hop_copy(which).wait_send()

    ends = shares + a_copies + beyond_copies + part_copies[0] + part_copies[1]
    ends = ends + core_copies + z_copies
    for copy in ends + list(y_copies.values()) + list(x_copies.values()):
        copy.wait_send()


def finish(hidden, grad, w, hidden_out, grad_out, w_out):
    hidden_out[...] = hidden[...]
    grad_out[...] = grad[...]
    w_out[...] = w[...]


def shards(
    cells_next, node_embed, enc_mix, out_cotangent, decoded_saved, dec_proj, tile_source, tile_codes
):
    hbm = pl.BlockSpec(memory_space=pl.ANY)
    vmem = pl.BlockSpec(memory_space=pltpu.VMEM)
    smem = pl.BlockSpec(memory_space=pltpu.SMEM)
    dma = pltpu.SemaphoreType.DMA
    scratch = [
        pltpu.SMEM((8, BLK), jnp.int32),
        pltpu.VMEM((8, BLK), jnp.int32),
        pltpu.VMEM((TILES, BLK, BLK), jnp.int32),
        pltpu.VMEM((2, 4, 4, BLK, CH), BF),
        pltpu.VMEM((2, 4, 4, BLK, CH), BF),
        pltpu.VMEM((4, 4, BLK, CH), BF),
        pltpu.VMEM((4, 4, BLK, CH), BF),
        pltpu.VMEM((4 * CH, CH), BF),
        pltpu.VMEM((4 * CH, CH), BF),
        pltpu.VMEM((NODES, CH), BF),
        pltpu.VMEM((Z_SLOTS + T2, 2, BLK, BLK), BF),
        pltpu.VMEM((SLOTS, 2, BLK, BLK), BF),
        pltpu.VMEM((Z_SLOTS, 2, BLK, BLK), BF),
        pltpu.VMEM((SLOTS, 2, BLK, BLK), BF),
        pltpu.VMEM((T2, 2, BLK, BLK), BF),
        pltpu.VMEM((2, NODES, SLOTS * BLK), BF),
        pltpu.VMEM((2, SLOTS * BLK, CH), BF),
        pltpu.VMEM((2, NODES, CH), F32),
        pltpu.VMEM((2, NODES, CH), F32),
        pltpu.VMEM((2, NODES, CH), BF),
        pltpu.VMEM((2, NODES, CH), BF),
        pltpu.VMEM((2, 2, NODES, CH), BF),
        pltpu.VMEM((2, 2, NODES, CH), BF),
        pltpu.VMEM((4, 2, NODES, CH), BF),
        pltpu.VMEM((4, 2, 4, 32, 4 * CH), F32),
        pltpu.VMEM((4, 4, 32, 4 * CH), F32),
        pltpu.VMEM((4, 4, 32, 4 * CH), F32),
        pltpu.VMEM((4, 4, 32, 4 * CH), BF),
        pltpu.VMEM((4, 3, 32, 4 * CH), BF),
        pltpu.VMEM((3, 32, 4 * CH), BF),
        pltpu.VMEM((3, 32, 4 * CH), BF),
        pltpu.VMEM((2, 4, 16, CH), F32),
        pltpu.VMEM((7, 16, CH), F32),
        dma((9,)),
        dma((2,)),
        dma((2,)),
        dma((8,)),
        dma((8,)),
        dma((8,)),
        dma((8,)),
        dma((8,)),
        dma((8,)),
        dma,
        dma,
        dma((2, 6)),
        dma((2, 6)),
        dma((4,)),
        dma((4,)),
        dma((4, 3)),
        dma((4, 3)),
        dma((3,)),
        dma((3,)),
        dma((7,)),
        dma((7,)),
        dma((2,)),
        dma((2,)),
        dma((2, 2)),
        dma((2, 2)),
        dma((3, 2)),
        dma((3, 2)),
        dma((2,)),
    ]
    results = pl.pallas_call(
        kernel,
        out_shape=(
            jax.ShapeDtypeStruct((NODES, CH), BF),
            jax.ShapeDtypeStruct((NODES, CH), BF),
            jax.ShapeDtypeStruct((16, CH), F32),
        ),
        in_specs=[smem] + [hbm] * 7,
        out_specs=(vmem, vmem, vmem),
        scratch_shapes=scratch,
        compiler_params=pltpu.CompilerParams(
            collective_id=0, has_side_effects=True, vmem_limit_bytes=60 * 1024 * 1024
        ),
        name="encode_and_backward",
    )(
        tile_source.T,
        cells_next.reshape(4, 4, BLK, CH),
        node_embed,
        enc_mix,
        out_cotangent.reshape(4, 4, BLK, CH),
        decoded_saved.reshape(4, 4, BLK, CH),
        dec_proj,
        tile_codes.reshape(TILES, BLK, BLK),
    )
    return pl.pallas_call(
        finish,
        out_shape=tuple(jax.ShapeDtypeStruct(r.shape, r.dtype) for r in results),
        in_specs=[vmem] * 3,
        out_specs=(vmem, vmem, vmem),
        name="finish",
    )(*results)


def solution(mesh):
    in_specs = (
        P("band", "chan"),
        P("band", "chan"),
        P(None, "chan"),
        P("band", "chan"),
        P("band", "chan"),
        P(None, "chan"),
        P(),
        P("band", None, None, None),
    )
    out_specs = (P("band", "chan"), P("band", "chan"), P("band", "chan"))
    return jax.shard_map(shards, mesh=mesh, in_specs=in_specs, out_specs=out_specs, check_vma=False)
```

```python
import jax
import jax.numpy as jnp
from jax import lax
from jax.experimental import pallas as pl
from jax.experimental.pallas import tpu as pltpu
from jax.sharding import PartitionSpec as P

BLK = 128
K = 16
NB_DEV = 2
CHIPS = 32
TILES = NB_DEV * K
SLOTS = 16
T2 = 8
CH = 256
COLS = 512
ROWS = 2048
QROWS = 512
NODES = 256
SCALE = (3.0 / (K * BLK)) ** 0.5 / 128.0
MESH = pl.DeviceIdType.MESH
BF = jnp.bfloat16
F32 = jnp.float32

Z_SLOTS = 24
CHUNK = 2
STEPS = 8
SHORT = 4
A_FIRST = 4
A_TICKS = (1, 1, 1, 1, 1, 1, 1, 1, 0)
TWO_TICK = 4
OWN_TICK = 5
BEYOND_TICK = 7


def chip_links(chip, z_hi, core):
    side = 1 - 2 * z_hi
    across = chip + side
    beyond = (chip - side + CHIPS) % CHIPS
    relay_to = (chip + 2 * side + CHIPS) % CHIPS
    two_to = (chip + 4 * core - 2 + CHIPS) % CHIPS
    two_from = (chip - 4 * core + 2 + CHIPS) % CHIPS
    return across, beyond, relay_to, two_to, two_from


def kernel(
    source,
    cells_hbm,
    embed_hbm,
    mix_hbm,
    cot_hbm,
    saved_hbm,
    proj_hbm,
    codes_hbm,
    hidden_out,
    grad_out,
    w_out,
    table,
    table_rows,
    codes,
    cells,
    cot,
    cot_all,
    saved_all,
    mix,
    proj,
    embed,
    packed,
    own_packed,
    got_z,
    got_y,
    got_two,
    lhs,
    rhs,
    own_sum,
    side_sum,
    beyond_send,
    beyond_recv,
    part_send,
    part_recv,
    agg_all,
    w_part,
    core_recv,
    y_own,
    y_send,
    y_recv,
    x_send,
    x_recv,
    wide_own,
    wide_send,
    wide_recv,
    last_send,
    last_recv,
    z_send,
    z_recv,
    load_sem,
    share_send,
    share_recv,
    up_send,
    up_recv,
    down_send,
    down_recv,
    relay_send,
    relay_recv,
    two_send,
    two_recv,
    a_send,
    a_recv,
    core_send_sem,
    core_recv_sem,
    y_send_sem,
    y_recv_sem,
    x_send_sem,
    x_recv_sem,
    wide_send_sem,
    wide_recv_sem,
    last_send_sem,
    last_recv_sem,
    z_send_sem,
    z_recv_sem,
    beyond_send_sem,
    beyond_recv_sem,
    part_send_sem,
    part_recv_sem,
    agg_send_sem,
    agg_recv_sem,
    hop_send_sem,
):
    band = lax.axis_index("band")
    q = lax.axis_index("chan")
    core = band % 2
    chip = band // 2
    h = chip % 2
    y = (band // 4) % 4
    x = band // 16
    across, beyond, relay_to, two_to, two_from = chip_links(chip, h, core)

    def at_chip(other_chip, chan):
        return (2 * other_chip + core, chan)

    def remote(src, dst, send, recv, device):
        return pltpu.make_async_remote_copy(
            src_ref=src,
            dst_ref=dst,
            send_sem=send,
            recv_sem=recv,
            device_id=device,
            device_id_type=MESH,
        )

    sibling = (band + 1 - 2 * core, q)
    across_q = [at_chip(across, (q + d) % 4) for d in range(4)]
    along_q = [(band, (q + d) % 4) for d in range(1, 4)]
    along_y = [(x * 16 + ((y + d) % 4) * 4 + h * 2 + core, q) for d in range(1, 4)]
    along_x = [(((x + d) % 4) * 16 + y * 4 + h * 2 + core, q) for d in range(1, 4)]

    barrier = pltpu.get_barrier_semaphore()
    partners = (
        [sibling]
        + across_q
        + along_q
        + along_y
        + along_x
        + [at_chip(two_to, q), at_chip(two_from, q)]
    )
    for partner in partners:
        pl.semaphore_signal(barrier, inc=1, device_id=partner, device_id_type=MESH)

    loads = [
        pltpu.make_async_copy(codes_hbm, codes, load_sem.at[0]),
        pltpu.make_async_copy(cells_hbm, cells.at[core], load_sem.at[1]),
        pltpu.make_async_copy(cot_hbm, cot.at[core], load_sem.at[2]),
        pltpu.make_async_copy(cot_hbm.at[q], cot_all.at[q], load_sem.at[3]),
        pltpu.make_async_copy(saved_hbm.at[q], saved_all.at[q], load_sem.at[4]),
        pltpu.make_async_copy(mix_hbm, mix, load_sem.at[5]),
        pltpu.make_async_copy(proj_hbm, proj, load_sem.at[6]),
        pltpu.make_async_copy(embed_hbm, embed, load_sem.at[7]),
    ]
    for load in loads:
        load.start()

    lane = lax.broadcasted_iota(jnp.int32, (8, BLK), 1)
    row = lax.broadcasted_iota(jnp.int32, (8, BLK), 0)

    def place(t, carry):
        rows, ranks = carry
        own, far, near, two = (
            source[t % K, 2 * owner + t // K]
            for owner in (band, 2 * beyond + core, 2 * across + core, 2 * two_from + core)
        )
        hits = (
            own // 32 == beyond,
            own // 32 == across,
            own // 32 == two_to,
            own // 32 == chip,
            far // 32 == chip,
            near // 32 == chip,
            two // 32 == chip,
        )
        half = 256 * (t // K) + 512
        entries = (
            (0, hits[0], ranks[0], t + 256),
            (0, hits[1], Z_SLOTS - 1 - ranks[1], t + 256),
            (2, hits[2], ranks[2], t + 256),
            (3, hits[3], ranks[3], t + 256),
            (4, hits[4], ranks[4], far % 32 + half + 1024 * ranks[4]),
            (5, hits[5], ranks[5], near % 32 + half + 1024 * (Z_SLOTS - 1 - ranks[5])),
            (6, hits[6], ranks[6], two % 32 + half + 1024 * ranks[6]),
            (7, hits[3], ranks[3], own % 32 + half + 1024 * ranks[3]),
        )
        for index, hit, slot, value in entries:
            spot = (row == index) & (lane == jnp.where(hit, slot, -1))
            rows = jnp.where(spot, value, rows)
        ranks = tuple(rank + jnp.where(hit, 1, 0) for rank, hit in zip(ranks, hits))
        return rows, ranks

    def pack(row, count, dest, base):
        def one(s, carry):
            item = table[row, s]
            words = codes[item & 31]
            low = ((words & 255) - 128).astype(F32)
            high = ((words >> 8) - 128).astype(F32)
            keep = jnp.where(item >= 256, 1.0, 0.0).astype(F32)
            dest[base + s, 0] = (low * keep).astype(BF)
            dest[base + s, 1] = (high * keep).astype(BF)
            return carry

        lax.fori_loop(0, count, one, 0)

    a_copies = []
    for half in range(2):
        for d in (1, 3, 2):
            other = (q + d) % 4
            for array, (src, dst) in enumerate(((cot_hbm, cot_all), (saved_hbm, saved_all))):
                index = 2 * (d - 1) + array
                part = pl.ds(2 * half, 2)
                a_copies.append(
                    remote(
                        src.at[other, part],
                        dst.at[q, part],
                        a_send.at[half, index],
                        a_recv.at[half, index],
                        (band, other),
                    )
                )
    waiting = list(a_copies)

    zero = jnp.int32(0)
    table_rows[...] = lax.fori_loop(
        0, TILES, place, (jnp.zeros((8, BLK), jnp.int32), (zero,) * 7)
    )[0]
    table_load = pltpu.make_async_copy(table_rows, table, load_sem.at[8])

    pl.semaphore_wait(barrier, len(partners))
    for _ in range(A_FIRST):
        waiting.pop(0).start()
    table_load.start()
    loads[0].wait()
    table_load.wait()
    pack(0, Z_SLOTS, packed, 0)
    pack(2, T2, packed, Z_SLOTS)

    z_up = at_chip(jnp.where(q == 3, across, chip), (q + 1) % 4)
    z_down = at_chip(jnp.where(q == 0, across, chip), (q + 3) % 4)

    def up_part(step):
        return pl.ds(CHUNK * step + 8 * (step // SHORT), CHUNK)

    def down_part(step):
        return pl.ds(CHUNK * step + 8, CHUNK)

    def up_copy(step, src):
        part = up_part(step)
        return remote(src.at[part], got_z.at[part], up_send.at[step], up_recv.at[step], z_up)

    def down_copy(step, src):
        part = down_part(step)
        return remote(src.at[part], got_z.at[part], down_send.at[step], down_recv.at[step], z_down)

    def relay_copy(index, part):
        return remote(
            got_z.at[part],
            got_y.at[part],
            relay_send.at[index],
            relay_recv.at[index],
            at_chip(relay_to, q),
        )

    for step in range(STEPS):

        @pl.when(q == 3)
        def _(step=step):
            up_copy(step, packed).start()

        @pl.when(q == 0)
        def _(step=step):
            down_copy(step, packed).start()

    two = remote(packed.at[pl.ds(Z_SLOTS, T2)], got_two, two_send, two_recv, at_chip(two_to, q))
    two.start()
    shares = [
        remote(cells_hbm, cells.at[core], share_send.at[0], share_recv.at[0], sibling),
        remote(cot_hbm, cot.at[core], share_send.at[1], share_recv.at[1], sibling),
    ]
    for share in shares:
        share.start()

    def sums(row, count, tiles):
        def one(s, carry):
            item = table[row, s]
            column = pl.ds(pl.multiple_of(s * BLK, BLK), BLK)
            first = jnp.where((item & 768) == 512, 1.0, 0.0).astype(BF)
            second = jnp.where((item & 768) == 768, 1.0, 0.0).astype(BF)
            for which in range(2):
                tile = tiles[item // 1024, which]
                lhs[which, pl.ds(0, BLK), column] = tile * first
                lhs[which, pl.ds(BLK, BLK), column] = tile * second
            block = item & 31
            rhs[0, column, :] = cells[block // 16, (block // 4) % 4, block % 4]
            rhs[1, column, :] = cot[block // 16, (block // 4) % 4, block % 4]
            return carry

        lax.fori_loop(0, count, one, 0)
        depth = count * BLK
        return [
            jnp.dot(
                lhs[which, :, pl.ds(0, depth)],
                rhs[which, pl.ds(0, depth), :],
                preferred_element_type=F32,
            )
            for which in range(2)
        ]

    beyond_copies = [
        remote(
            beyond_send.at[which],
            beyond_recv.at[which],
            beyond_send_sem.at[which],
            beyond_recv_sem.at[which],
            at_chip((chip - 2 * (1 - 2 * h) + CHIPS) % CHIPS, q),
        )
        for which in range(2)
    ]

    def send_beyond():
        for step in range(4):
            relay_copy(step, up_part(step)).wait_recv()
            relay_copy(step + 4, down_part(step)).wait_recv()
        result = sums(4, SLOTS, got_y)
        for which in range(2):
            beyond_send[which] = result[which].astype(BF)
            beyond_copies[which].start()

    part_copies = [
        [
            remote(
                part_send.at[g, which],
                part_recv.at[g, which],
                part_send_sem.at[g, which],
                part_recv_sem.at[g, which],
                at_chip(to, q),
            )
            for which in range(2)
        ]
        for g, to in enumerate((across, two_from))
    ]

    def send_two():
        two.wait_recv()
        result = sums(6, T2, got_two)
        for which in range(2):
            part_send[1, which] = result[which].astype(BF)
            part_copies[1][which].start()

    def sum_own():
        pack(3, SLOTS, own_packed, 0)
        result = sums(7, SLOTS, own_packed)
        for which in range(2):
            own_sum[which] = result[which]

    core_copies = [
        remote(
            w_part.at[d, 1 - core],
            core_recv.at[d],
            core_send_sem.at[d],
            core_recv_sem.at[d],
            sibling,
        )
        for d in range(4)
    ]
    order = (1, 2, 3, 0)

    def start_projection():
        for load in loads[3:5]:
            load.wait()
        for copy in a_copies:
            copy.wait_recv()

        for d in order:
            left = cot_all.at[(x + d) % 4]

            def columns(j, carry, d=d, left=left):
                product = lax.dot_general(
                    left[...].reshape(QROWS, CH),
                    saved_all[j].reshape(QROWS, CH),
                    (((0,), (0,)), ((), ())),
                    preferred_element_type=F32,
                )
                span = pl.ds(pl.multiple_of(j * CH, CH), CH)
                for group in range(8):
                    for half in range(2):
                        start = (2 * group + half) * 16
                        w_part[d, half, group // 2, pl.ds((group % 2) * 16, 16), span] = product[
                            start : start + 16
                        ]
                return carry

            lax.fori_loop(0, 4, columns, 0)
            core_copies[d].start()

    for tick in range(STEPS + 1):
        if tick == TWO_TICK:
            for load in loads[1:3]:
                load.wait()
            for share in shares:
                share.wait_recv()
            send_two()
        if tick == OWN_TICK:
            sum_own()
        if tick == BEYOND_TICK:
            send_beyond()
        up, down = tick - q, tick - 3 + q

        @pl.when((up >= 0) & (up < STEPS) & ((up < SHORT) | (q < 2)))
        def _(step=up):
            up_copy(step, got_z).wait_recv()

            @pl.when((q < 3) & ((step < SHORT) | (q < 1)))
            def _():
                up_copy(step, got_z).start()

            @pl.when(step < 4)
            def _():
                relay_copy(step, up_part(step)).start()

        @pl.when((down >= 0) & (down < STEPS) & ((down < SHORT) | (q > 1)))
        def _(step=down):
            down_copy(step, got_z).wait_recv()

            @pl.when((q > 0) & ((step < SHORT) | (q > 2)))
            def _():
                down_copy(step, got_z).start()

            @pl.when(step < 4)
            def _():
                relay_copy(step + 4, down_part(step)).start()

        for _ in range(A_TICKS[tick]):
            waiting.pop(0).start()

    result = sums(5, SLOTS, got_z)
    for which in range(2):
        side_sum[which] = result[which]
    for which in range(2):
        beyond_copies[which].wait_recv()
        total = side_sum[which] + beyond_recv[which].astype(F32)
        part_send[0, which] = total.astype(BF)
        part_copies[0][which].start()
    for copy in waiting:
        copy.start()
    start_projection()

    def agg_copy(d, which):
        return remote(
            agg_all.at[q, which],
            agg_all.at[q, which],
            agg_send_sem.at[d - 1, which],
            agg_recv_sem.at[d - 1, which],
            (band, (q + d) % 4),
        )

    def hop_copy(which):
        block = (q + 2) % 4
        return remote(
            agg_all.at[block, which],
            agg_all.at[block, which],
            hop_send_sem.at[which],
            agg_recv_sem.at[2 * (q - 1), which],
            (band, 3 * (q - 1)),
        )

    middle = (q == 1) | (q == 2)

    def far(d):
        return ((q == 0) & (d == 3)) | ((q == 3) & (d == 1))

    for which in range(2):
        total = own_sum[which]
        for g in range(2):
            part_copies[g][which].wait_recv()
            total = total + part_recv[g, which].astype(F32)
        agg_all[q, which] = (total * SCALE).astype(BF)
        for d in (2, 1, 3):

            @pl.when(jnp.logical_not(far(d)))
            def _(d=d, which=which):
                agg_copy(d, which).start()

    y_copies = {}
    wide_copies = {}
    for d in order:
        core_copies[d].wait_recv()
        for yy in range(4):
            total = w_part[d, core, yy] + core_recv[d, yy]
            y_own[d, yy] = total[:, :COLS]
            y_send[d, yy] = total[:, :COLS].astype(BF)
            if d > 0:
                wide_send[d - 1, yy] = total[:, COLS:].astype(BF)
            else:
                wide_own[yy] = total[:, COLS:]
        if d > 0:
            wide_copies[d] = remote(
                wide_send.at[d - 1],
                wide_recv.at[d - 1],
                wide_send_sem.at[d - 1],
                wide_recv_sem.at[d - 1],
                along_x[d - 1],
            )
            wide_copies[d].start()
        for e in range(1, 4):
            y_copies[d, e] = remote(
                y_send.at[d, (y + e) % 4],
                y_recv.at[d, e - 1],
                y_send_sem.at[d, e - 1],
                y_recv_sem.at[d, e - 1],
                along_y[e - 1],
            )
            y_copies[d, e].start()

    last_copies = {}
    for d in range(1, 4):
        wide_copies[d].wait_recv()
    for yy in range(4):
        total = wide_own[yy]
        for d in range(1, 4):
            total = total + wide_recv[d - 1, yy].astype(F32)
        wide_own[yy] = total
        last_send[yy] = total.astype(BF)
    for e in range(1, 4):
        last_copies[e] = remote(
            last_send.at[(y + e) % 4],
            last_recv.at[e - 1],
            last_send_sem.at[e - 1],
            last_recv_sem.at[e - 1],
            along_y[e - 1],
        )
        last_copies[e].start()
    x_copies = {}
    for d in order:
        total = y_own[d, y]
        for e in range(1, 4):
            y_copies[d, e].wait_recv()
            total = total + y_recv[d, e - 1].astype(F32)
        if d > 0:
            x_send[d - 1] = total.astype(BF)
            x_copies[d] = remote(
                x_send.at[d - 1],
                x_recv.at[d - 1],
                x_send_sem.at[d - 1],
                x_recv_sem.at[d - 1],
                along_x[d - 1],
            )
            x_copies[d].start()
    for which in range(2):
        agg_copy(2, which).wait_recv()

        @pl.when(middle)
        def _(which=which):
            hop_copy(which).start()

    other = wide_own[y]
    for d in range(1, 4):
        x_copies[d].wait_recv()
        total = total + x_recv[d - 1].astype(F32)
        last_copies[d].wait_recv()
        other = other + last_recv[d - 1].astype(F32)
    for hh in range(2):
        rows = slice(hh * 16, hh * 16 + 16)
        for qq in range(2):
            span = slice(qq * CH, qq * CH + CH)
            z_send[hh, qq] = total[rows, span]
            z_send[hh, qq + 2] = other[rows, span]
    z_copies = []
    for hd in range(2):
        for qd in range(4):
            if hd + qd > 0:
                index = hd * 4 + qd - 1
                chan = (q + qd) % 4
                device = at_chip(across, chan) if hd else (band, chan)
                to_h = 1 - h if hd else h
                z_copies.append(
                    remote(
                        z_send.at[to_h, chan],
                        z_recv.at[index],
                        z_send_sem.at[index],
                        z_recv_sem.at[index],
                        device,
                    )
                )
    for copy in z_copies:
        copy.start()

    for load in loads[5:8]:
        load.wait()
    for d in (1, 3):
        agg_copy(d, 0).wait_recv()
    mixed = jnp.zeros((NODES, CH), F32)
    grad = jnp.zeros((NODES, CH), F32)
    for j in range(4):
        mixed = mixed + jnp.dot(
            agg_all[j, 0], mix[pl.ds(j * CH, CH), :], preferred_element_type=F32
        )
    hidden_out[...] = (embed[...].astype(F32) + mixed / (1.0 + jnp.exp(-mixed))).astype(BF)
    for d in (1, 3):
        agg_copy(d, 1).wait_recv()
    for j in range(4):
        grad = grad + jnp.dot(
            agg_all[j, 1], proj[pl.ds(j * CH, CH), :], preferred_element_type=F32
        )
    grad_out[...] = grad.astype(BF)

    total = z_send[h, q]
    for index, copy in enumerate(z_copies):
        copy.wait_recv()
        total = total + z_recv[index]
    w_out[...] = total * (ROWS * 64) ** (-0.5)

    for step in range(STEPS):

        @pl.when((q == 0) | (q == 3) | (step < SHORT))
        def _(step=step):
            up_copy(step, got_z).wait_send()
            down_copy(step, got_z).wait_send()

    for step in range(4):
        relay_copy(step, up_part(step)).wait_send()
        relay_copy(step + 4, down_part(step)).wait_send()
    two.wait_send()
    for which in range(2):
        for d in range(1, 4):

            @pl.when(jnp.logical_not(far(d)))
            def _(d=d, which=which):
                agg_copy(d, which).wait_send()

        @pl.when(middle)
        def _(which=which):
            hop_copy(which).wait_send()

    ends = shares + a_copies + beyond_copies + part_copies[0] + part_copies[1]
    ends = ends + core_copies + z_copies
    for some in (y_copies, x_copies, wide_copies, last_copies):
        ends = ends + list(some.values())
    for copy in ends:
        copy.wait_send()


def finish(hidden, grad, w, hidden_out, grad_out, w_out):
    hidden_out[...] = hidden[...]
    grad_out[...] = grad[...]
    w_out[...] = w[...]


def shards(
    cells_next, node_embed, enc_mix, out_cotangent, decoded_saved, dec_proj, tile_source, tile_codes
):
    hbm = pl.BlockSpec(memory_space=pl.ANY)
    vmem = pl.BlockSpec(memory_space=pltpu.VMEM)
    smem = pl.BlockSpec(memory_space=pltpu.SMEM)
    dma = pltpu.SemaphoreType.DMA
    scratch = [
        pltpu.SMEM((8, BLK), jnp.int32),
        pltpu.VMEM((8, BLK), jnp.int32),
        pltpu.VMEM((TILES, BLK, BLK), jnp.int32),
        pltpu.VMEM((2, 4, 4, BLK, CH), BF),
        pltpu.VMEM((2, 4, 4, BLK, CH), BF),
        pltpu.VMEM((4, 4, BLK, CH), BF),
        pltpu.VMEM((4, 4, BLK, CH), BF),
        pltpu.VMEM((4 * CH, CH), BF),
        pltpu.VMEM((4 * CH, CH), BF),
        pltpu.VMEM((NODES, CH), BF),
        pltpu.VMEM((Z_SLOTS + T2, 2, BLK, BLK), BF),
        pltpu.VMEM((SLOTS, 2, BLK, BLK), BF),
        pltpu.VMEM((Z_SLOTS, 2, BLK, BLK), BF),
        pltpu.VMEM((SLOTS, 2, BLK, BLK), BF),
        pltpu.VMEM((T2, 2, BLK, BLK), BF),
        pltpu.VMEM((2, NODES, SLOTS * BLK), BF),
        pltpu.VMEM((2, SLOTS * BLK, CH), BF),
        pltpu.VMEM((2, NODES, CH), F32),
        pltpu.VMEM((2, NODES, CH), F32),
        pltpu.VMEM((2, NODES, CH), BF),
        pltpu.VMEM((2, NODES, CH), BF),
        pltpu.VMEM((2, 2, NODES, CH), BF),
        pltpu.VMEM((2, 2, NODES, CH), BF),
        pltpu.VMEM((4, 2, NODES, CH), BF),
        pltpu.VMEM((4, 2, 4, 32, 4 * CH), F32),
        pltpu.VMEM((4, 4, 32, 4 * CH), F32),
        pltpu.VMEM((4, 4, 32, COLS), F32),
        pltpu.VMEM((4, 4, 32, COLS), BF),
        pltpu.VMEM((4, 3, 32, COLS), BF),
        pltpu.VMEM((3, 32, COLS), BF),
        pltpu.VMEM((3, 32, COLS), BF),
        pltpu.VMEM((4, 32, COLS), F32),
        pltpu.VMEM((3, 4, 32, COLS), BF),
        pltpu.VMEM((3, 4, 32, COLS), BF),
        pltpu.VMEM((4, 32, COLS), BF),
        pltpu.VMEM((3, 32, COLS), BF),
        pltpu.VMEM((2, 4, 16, CH), F32),
        pltpu.VMEM((7, 16, CH), F32),
        dma((9,)),
        dma((2,)),
        dma((2,)),
        dma((8,)),
        dma((8,)),
        dma((8,)),
        dma((8,)),
        dma((8,)),
        dma((8,)),
        dma,
        dma,
        dma((2, 6)),
        dma((2, 6)),
        dma((4,)),
        dma((4,)),
        dma((4, 3)),
        dma((4, 3)),
        dma((3,)),
        dma((3,)),
        dma((3,)),
        dma((3,)),
        dma((3,)),
        dma((3,)),
        dma((7,)),
        dma((7,)),
        dma((2,)),
        dma((2,)),
        dma((2, 2)),
        dma((2, 2)),
        dma((3, 2)),
        dma((3, 2)),
        dma((2,)),
    ]
    results = pl.pallas_call(
        kernel,
        out_shape=(
            jax.ShapeDtypeStruct((NODES, CH), BF),
            jax.ShapeDtypeStruct((NODES, CH), BF),
            jax.ShapeDtypeStruct((16, CH), F32),
        ),
        in_specs=[smem] + [hbm] * 7,
        out_specs=(vmem, vmem, vmem),
        scratch_shapes=scratch,
        compiler_params=pltpu.CompilerParams(
            collective_id=0, has_side_effects=True, vmem_limit_bytes=60 * 1024 * 1024
        ),
        name="encode_and_backward",
    )(
        tile_source.T,
        cells_next.reshape(4, 4, BLK, CH),
        node_embed,
        enc_mix,
        out_cotangent.reshape(4, 4, BLK, CH),
        decoded_saved.reshape(4, 4, BLK, CH),
        dec_proj,
        tile_codes.reshape(TILES, BLK, BLK),
    )
    return pl.pallas_call(
        finish,
        out_shape=tuple(jax.ShapeDtypeStruct(r.shape, r.dtype) for r in results),
        in_specs=[vmem] * 3,
        out_specs=(vmem, vmem, vmem),
        name="finish",
    )(*results)


def solution(mesh):
    in_specs = (
        P("band", "chan"),
        P("band", "chan"),
        P(None, "chan"),
        P("band", "chan"),
        P("band", "chan"),
        P(None, "chan"),
        P(),
        P("band", None, None, None),
    )
    out_specs = (P("band", "chan"), P("band", "chan"), P("band", "chan"))
    return jax.shard_map(shards, mesh=mesh, in_specs=in_specs, out_specs=out_specs, check_vma=False)
```
